16 devices in a mesh: rep: 1, r: 4 (over y, z), s: 4 (over x, core).
Axes of the slice: x: 2, y: 2, z: 2, core: 2. Of those that a mesh axis runs over, the one named last changes fastest.
Arguments:
- x: bfloat16 [16, 4096, 1024], P(('rep', 'r', 's'))
- dy: bfloat16 [16, 4096, 1024], P(('rep', 'r', 's'))
- w_gate: bfloat16 [2, 1024, 3200], P(None, 's')
- w_up: bfloat16 [2, 1024, 3200], P(None, 's')
- w_down: bfloat16 [2, 3200, 1024], P(None, 's')
Outputs:
- output 1: bfloat16 [16, 4096, 1024], P(('rep', 'r', 's'))
- output 2: bfloat16 [2, 1024, 3200], P('rep', 's')
- output 3: bfloat16 [2, 1024, 3200], P('rep', 's')
- output 4: bfloat16 [2, 3200, 1024], P('rep', 's')
All inputs are finite; a program needn't handle non-finite values.
Results may differ from the reference program's by a relative error of at most 0.018.
Values are sent between devices in bfloat16 or wider.
A program may use at most 2 GiB of HBM per device.

```python
import jax
import jax.numpy as jnp
from jax import lax

SEQUENCES = 16
TOKENS = 4096
D = 1024
FF = 3200
LAYERS = 2
NAMES = ("w_gate", "w_up", "w_down")
SHAPES = {"w_gate": (LAYERS, D, FF), "w_up": (LAYERS, D, FF), "w_down": (LAYERS, FF, D)}


def bump(key, n, height):
    away = (jnp.arange(n, dtype=jnp.int32) - jax.random.randint(key, (), 0, n, jnp.int32)) % n
    return jnp.where(away < n // 8, height, 1.0)


def together(key, own, strength):
    shared = jax.random.normal(key, own.shape[1:], jnp.float32)
    return (own + strength * shared) * lax.rsqrt(1 + strength * strength)


def setup_inputs(seed: int = 0, part: int = 0) -> dict:
    kx, kdy, ka, kb, kz, kf, kh, kl, *kw = jax.random.split(jax.random.key(seed), 8 + len(NAMES))
    kx, kdy, ka, kb = (jax.random.fold_in(k, part) for k in (kx, kdy, ka, kb))
    shape = (SEQUENCES, TOKENS, D)
    much_x, much_dy = jax.random.uniform(kz, (2,), jnp.float32, 0.0, 1.0)
    layers = 2.0 ** jax.random.uniform(kl, (LAYERS, 1, 1), jnp.float32, -1.0, 1.0)
    x = together(ka, jax.random.normal(kx, shape, jnp.float32), much_x) * bump(kf, D, 4.0)
    dy = together(kb, jax.random.normal(kdy, shape, jnp.float32), much_dy)
    drawn = {"x": x.astype(jnp.bfloat16), "dy": (dy * (SEQUENCES * TOKENS) ** -0.5).astype(jnp.bfloat16)}
    for key, name in zip(kw, NAMES, strict=True):
        w = jax.random.normal(key, SHAPES[name], jnp.float32) * SHAPES[name][1] ** -0.5
        drawn[name] = (w * {"w_gate": 1.0, "w_up": bump(kh, FF, 4.0), "w_down": layers}[name]).astype(jnp.bfloat16)
    return drawn


def matmul(a, w):
    return jnp.dot(a, w, preferred_element_type=jnp.float32).astype(jnp.bfloat16)


def normed(h):
    wide = h.astype(jnp.float32)
    scale = lax.rsqrt(jnp.mean(wide**2, -1, keepdims=True) + 1e-6)
    return (wide * scale).astype(jnp.bfloat16)


def layer(h, w):
    a = normed(h)
    gate = jnp.dot(a, w["w_gate"], preferred_element_type=jnp.float32)
    up = jnp.dot(a, w["w_up"], preferred_element_type=jnp.float32)
    return h + matmul((jax.nn.silu(gate) * up).astype(jnp.bfloat16), w["w_down"])


def stack(weights, h):
    return lax.scan(lambda h, w: (layer(h, w), None), h, weights)[0]


def reference(x, dy, w_gate, w_up, w_down):
    weights = dict(zip(NAMES, (w_gate, w_up, w_down), strict=True))

    def take(so_far, sequence):
        h, by_y = sequence
        _, back = jax.vjp(stack, weights, h)
        by_weights, by_h = back(by_y)
        return jax.tree.map(lambda total, term: total + term.astype(jnp.float32), so_far, by_weights), by_h

    none_yet = {name: jnp.zeros(w.shape, jnp.float32) for name, w in weights.items()}
    by_weights, by_x = lax.scan(take, none_yet, (x, dy))
    return (by_x, *(by_weights[name].astype(jnp.bfloat16) for name in NAMES))
```

```python
import functools

import jax
import jax.numpy as jnp
from jax import lax
from jax.experimental import pallas as pl
from jax.experimental.pallas import tpu as pltpu
from jax.sharding import PartitionSpec as P

BF, F32 = jnp.bfloat16, jnp.float32
MESH = pl.DeviceIdType.MESH
NT = (((1,), (1,)), ((), ()))
TN = (((0,), (0,)), ((), ()))
ANY = pl.BlockSpec(memory_space=pl.ANY)
CHUNKS = 5
VMEM_LIMIT = 67043328


def dot(a, b, dims=(((1,), (0,)), ((), ()))):
    return lax.dot_general(a, b, dims, preferred_element_type=F32)


def scale_of(wide):
    return lax.rsqrt(jnp.mean(wide * wide, -1, keepdims=True) + 1e-6)


def pieces(width):
    first = 256 if width > 512 else width // 2
    return ((0, first), (first, width - first))


def rows(start, size, unit=16):
    return pl.ds(pl.multiple_of(start, unit) if size % unit == 0 else start, size)


def gate_up_kernel(x_ref, wg_ref, wu_ref, a_ref, hid_ref, g_ref, u_ref):
    wide = x_ref[...].astype(F32)
    a = (wide * scale_of(wide)).astype(BF)
    a_ref[...] = a
    width = wg_ref.shape[1] // CHUNKS
    for j in range(CHUNKS):
        c = pl.ds(j * width, width)
        both = dot(a, jnp.concatenate([wg_ref[:, c], wu_ref[:, c]], 1))
        g, u = both[:, :width], both[:, width:]
        g_ref[:, c], u_ref[:, c] = g, u
        hid_ref[:, c] = (g * jax.nn.sigmoid(g) * u).astype(BF)


def gate_up(x, wg, wu):
    t, d = x.shape
    f = wg.shape[1]
    tm = t // 16
    whole = pl.BlockSpec((d, f), lambda i: (0, 0), pipeline_mode=pl.Buffered(1))
    part = lambda n: pl.BlockSpec((tm, n), lambda i: (i, 0))
    return pl.pallas_call(
        gate_up_kernel,
        grid=(t // tm,),
        in_specs=[part(d), whole, whole],
        out_specs=[part(d), part(f), part(f), part(f)],
        out_shape=[jax.ShapeDtypeStruct((t, n), k) for n, k in ((d, BF), (f, BF), (f, F32), (f, F32))],
        compiler_params=pltpu.CompilerParams(vmem_limit_bytes=VMEM_LIMIT, dimension_semantics=("arbitrary",)),
        cost_estimate=pl.CostEstimate(flops=4 * t * d * f, bytes_accessed=12 * t * f, transcendentals=t * f),
        name="gate_up",
    )(x, wg, wu)


def down_kernel(hid_ref, w_ref, x_ref, h_ref, a_ref):
    h = (x_ref[...].astype(F32) + dot(hid_ref[...], w_ref[...]).astype(BF).astype(F32)).astype(BF)
    h_ref[...] = h
    wide = h.astype(F32)
    a_ref[...] = (wide * scale_of(wide)).astype(BF)


def down(hid, w, x):
    t, d = x.shape
    f = w.shape[0]
    tm = t // 8
    part = lambda n: pl.BlockSpec((tm, n), lambda i: (i, 0))
    return pl.pallas_call(
        down_kernel,
        grid=(t // tm,),
        in_specs=[part(f), pl.BlockSpec((f, d), lambda i: (0, 0), pipeline_mode=pl.Buffered(1)), part(d)],
        out_specs=[part(d), part(d)],
        out_shape=[jax.ShapeDtypeStruct((t, d), BF)] * 2,
        compiler_params=pltpu.CompilerParams(vmem_limit_bytes=VMEM_LIMIT, dimension_semantics=("arbitrary",)),
        cost_estimate=pl.CostEstimate(flops=2 * t * d * f, bytes_accessed=2 * t * f, transcendentals=0),
        name="down",
    )(hid, w, x)


def here():
    s = lax.axis_index("s")
    return lax.axis_index("r"), lax.div(s, 2), lax.rem(s, 2)


def send(src, dst, sems, to):
    return pltpu.make_async_remote_copy(
        src_ref=src, dst_ref=dst, send_sem=sems[0], recv_sem=sems[1], device_id=to, device_id_type=MESH
    )


def start(copies):
    for copy in copies:
        copy.start()


def wait(copies):
    for copy in copies:
        copy.wait()


def backward_kernel(saved, *refs):
    n_in = 8 if saved else 6
    a_hbm, h_hbm, dy_hbm, wg_hbm, wu_hbm, wd_hbm = refs[:6]
    g_hbm, u_hbm = refs[6:n_in] if saved else (None, None)
    out_hbm, og_hbm, ou_hbm, od_hbm, dgu_hbm, dwd_hbm = refs[n_in : n_in + 6]
    (stg, buf_d, acc, buf_x, s_x, s_r, buf_r, s_g, sem_d, sem_x, sem_r, sem_g, sem_gl, free_d, free_x, free_r, entered) = refs[n_in + 6 :]

    t, d = a_hbm.shape
    f = wd_hbm.shape[0]
    c = f // CHUNKS
    own = d // 4
    quarter = own // 4
    own_d = f // 4
    rd = own_d // 5
    qd = d // 4
    me_r, x, core = here()
    partner = {"s": x * 2 + (1 - core)}
    across = {"s": (1 - x) * 2 + core}
    peers = [(lax.rem(me_r + k, 4), {"r": lax.rem(me_r + k, 4)}) for k in (1, 2, 3)]
    everyone = [partner, across] + [p for _, p in peers]

    barrier = pltpu.get_barrier_semaphore()
    for p in everyone:
        pl.semaphore_signal(barrier, inc=1, device_id=p, device_id_type=MESH)
    pl.semaphore_wait(barrier, 5)

    def d_copies():
        return [
            send(stg.at[rows((2 * k + 1 - core) * own, own), :], buf_d.at[k], (sem_d.at[0, k], sem_d.at[1, k]), partner)
            for k in range(2)
        ]

    def x_copies():
        return [send(s_x, buf_x, (sem_x.at[0], sem_x.at[1]), across)]

    def r_copies():
        return [
            send(s_r.at[rows(n * quarter, quarter), :], buf_r.at[k], (sem_r.at[0, k], sem_r.at[1, k]), p)
            for k, (n, p) in enumerate(peers)
        ]

    def g_copies(p):
        at = (rows(me_r * quarter, quarter), rows(p * c, c, 128))
        far = [
            send(s_g.at[:, pl.ds(i * c, c)], o.at[at], (sem_g.at[0, lax.rem(p, 2), i, k], sem_g.at[1, lax.rem(p, 2), i, k]), to)
            for k, (_, to) in enumerate(peers)
            for i, o in enumerate((og_hbm, ou_hbm))
        ]
        near = [pltpu.make_async_copy(s_g.at[:, pl.ds(i * c, c)], o.at[at], sem_gl.at[i]) for i, o in enumerate((og_hbm, ou_hbm))]
        return far + near

    def e0(p, first):
        if not first:
            pl.semaphore_wait(free_d, 1)
        start(d_copies())

    def e1(p, first, last):
        wait(d_copies())
        acc[lax.rem(p, 2)] = stg[rows((2 * x + core) * own, own), :].astype(F32) + buf_d[x].astype(F32)
        s_x[...] = (stg[rows((2 * (1 - x) + core) * own, own), :].astype(F32) + buf_d[1 - x].astype(F32)).astype(BF)
        if not last:
            pl.semaphore_signal(free_d, inc=1, device_id=partner, device_id_type=MESH)
        if not first:
            pl.semaphore_wait(free_x, 1)
        start(x_copies())

    def e2(p, first, last):
        wait(x_copies())
        total = acc[lax.rem(p, 2)] + buf_x[...].astype(F32)
        acc[lax.rem(p, 2)] = total
        s_r[...] = total.astype(BF)
        if not last:
            pl.semaphore_signal(free_x, inc=1, device_id=across, device_id_type=MESH)
        if not first:
            for k in range(3):
                pl.semaphore_wait(free_r.at[k], 1)
        start(r_copies())

    def e3(p, last):
        wait(r_copies())
        total = acc[lax.rem(p, 2), rows(me_r * quarter, quarter), :]
        for k in range(3):
            total = total + buf_r[k].astype(F32)
        s_g[...] = total.astype(BF)
        if not last:
            for k, (_, to) in enumerate(peers):
                pl.semaphore_signal(free_r.at[2 - k], inc=1, device_id=to, device_id_type=MESH)
        start(g_copies(p))

    def e4(p):
        wait(g_copies(p))

    tm = t // 8 if saved else t // 4
    tiles = t // tm

    def chunks(*bufs):
        if saved:
            a_v, dy_v, wd_v, hid_v, dgs, dst, g_v, u_v, sem_a, sem_w, sem_o, sem_s = bufs
        else:
            a_v, dy_v, wd_v, hid_v, dgs, dst, wgu_v, sem_a, sem_w, sem_o = bufs

        def a_copies(i):
            at = rows(i * tm, tm)
            return [
                pltpu.make_async_copy(a_hbm.at[at, :], a_v.at[at, :], sem_a.at[0, i]),
                pltpu.make_async_copy(dy_hbm.at[at, :], dy_v.at[at, :], sem_a.at[1, i]),
            ]

        def w_copies(j):
            slot = lax.rem(j, 2)
            at = rows(j * c, c, 128)
            w = [pltpu.make_async_copy(wd_hbm.at[at, :], wd_v.at[slot], sem_w.at[slot, 0])]
            if not saved:
                w.append(pltpu.make_async_copy(wg_hbm.at[:, at], wgu_v.at[slot, :, pl.ds(0, c)], sem_w.at[slot, 1]))
                w.append(pltpu.make_async_copy(wu_hbm.at[:, at], wgu_v.at[slot, :, pl.ds(c, c)], sem_w.at[slot, 2]))
            return w

        def s_copies(n):
            slot = lax.rem(n, 2)
            at = (rows(lax.rem(n, tiles) * tm, tm), rows(lax.div(n, tiles) * c, c, 128))
            return [
                pltpu.make_async_copy(g_hbm.at[at], g_v.at[slot], sem_s.at[slot, 0]),
                pltpu.make_async_copy(u_hbm.at[at], u_v.at[slot], sem_s.at[slot, 1]),
            ]

        def o_copies(j):
            return [
                pltpu.make_async_copy(dgs.at[:, pl.ds(0, c)], dgu_hbm.at[:, rows(j * c, c, 128)], sem_o.at[0]),
                pltpu.make_async_copy(dgs.at[:, pl.ds(c, c)], dgu_hbm.at[:, rows(f + j * c, c, 128)], sem_o.at[1]),
            ]

        def dw_copy(j):
            return [pltpu.make_async_copy(dst, dwd_hbm.at[rows(j * c, c), :], sem_o.at[2])]

        start(w_copies(0))
        if saved:
            start(s_copies(0))
        for i in range(tiles):
            start(a_copies(i))

        def chunk(j, _):
            slot = lax.rem(j, 2)

            @pl.when(j >= 3)
            def _():
                e4(j - 3)

            @pl.when(j == 2)
            def _():
                e2(j - 2, True, False)

            @pl.when(j >= 3)
            def _():
                e2(j - 2, False, False)

            @pl.when(j == 1)
            def _():
                e0(j - 1, True)

            @pl.when(j >= 2)
            def _():
                e0(j - 1, False)

            @pl.when(j >= 1)
            def _():
                wait(o_copies(j - 1))

            wait(w_copies(j))

            @pl.when(j + 1 < CHUNKS)
            def _():
                start(w_copies(j + 1))

            def tile(i, _):
                @pl.when(j == 0)
                def _():
                    wait(a_copies(i))

                if saved:
                    n = j * tiles + i

                    @pl.when(n + 1 < CHUNKS * tiles)
                    def _():
                        start(s_copies(n + 1))

                    wait(s_copies(n))

                @pl.when(jnp.logical_and(i == tiles // 2, j == 1))
                def _():
                    e1(j - 1, True, False)

                @pl.when(jnp.logical_and(i == tiles // 2, j >= 2))
                def _():
                    e1(j - 1, False, False)

                r = rows(i * tm, tm)
                for p0, w in pieces(c):
                    if saved:
                        g = g_v[lax.rem(n, 2), :, pl.ds(p0, w)]
                        u = u_v[lax.rem(n, 2), :, pl.ds(p0, w)]
                    else:
                        a = a_v[r, :]
                        both = dot(a, jnp.concatenate([wgu_v[slot, :, pl.ds(p0, w)], wgu_v[slot, :, pl.ds(c + p0, w)]], 1))
                        g, u = both[:, :w], both[:, w:]
                    dh = dot(dy_v[r, :], wd_v[slot, pl.ds(p0, w), :], NT).astype(BF).astype(F32)
                    s = jax.nn.sigmoid(g)
                    silu = g * s
                    hid_v[r, pl.ds(p0, w)] = (silu * u).astype(BF)
                    dgs[r, pl.ds(c + p0, w)] = (dh * silu).astype(BF)
                    dgs[r, pl.ds(p0, w)] = (dh * u * (s + silu * (1.0 - s))).astype(BF)
                return 0

            lax.fori_loop(0, tiles, tile, 0)
            start(o_copies(j))

            @pl.when(j >= 1)
            def _():
                wait(dw_copy(j - 1))

            for p0, w in pieces(c):
                dst[pl.ds(p0, w), :] = dot(hid_v[:, pl.ds(p0, w)], dy_v[...], TN).astype(BF)
            start(dw_copy(j))

            @pl.when(j >= 2)
            def _():
                e3(j - 2, False)

            for k in range(2):
                stg[pl.ds(k * (d // 2), d // 2), :] = dot(a_v[:, pl.ds(k * (d // 2), d // 2)], dgs[...], TN).astype(BF)
            return 0

        lax.fori_loop(0, CHUNKS, chunk, 0)
        wait(o_copies(CHUNKS - 1))
        wait(dw_copy(CHUNKS - 1))

    bufs = [
        pltpu.VMEM((t, d), BF),
        pltpu.VMEM((t, d), BF),
        pltpu.VMEM((2, c, d), BF),
        pltpu.VMEM((t, c), BF),
        pltpu.VMEM((t, 2 * c), BF),
        pltpu.VMEM((c, d), BF),
    ]
    bufs += [pltpu.VMEM((2, tm, c), F32)] * 2 if saved else [pltpu.VMEM((2, d, 2 * c), BF)]
    bufs += [pltpu.SemaphoreType.DMA((2, tiles)), pltpu.SemaphoreType.DMA((2, 3)), pltpu.SemaphoreType.DMA((3,))]
    bufs += [pltpu.SemaphoreType.DMA((2, 2))] if saved else []
    pl.run_scoped(chunks, *bufs)

    ta = t // 8

    def last(wg_v, wu_v, dgu_v, h_v, dy_v, o_v, own_v, bd_v, ac_v, bx_v, sx_v, br_v, sg_v, sem_w, sem_i, sem_o, dd, dx, dr, dg, dl):
        def i_copies(i):
            slot = lax.rem(i, 2)
            at = rows(i * ta, ta)
            return [
                pltpu.make_async_copy(dgu_hbm.at[at, :], dgu_v.at[slot], sem_i.at[slot, 0]),
                pltpu.make_async_copy(h_hbm.at[at, :], h_v.at[slot], sem_i.at[slot, 1]),
                pltpu.make_async_copy(dy_hbm.at[at, :], dy_v.at[slot], sem_i.at[slot, 2]),
            ]

        def o_copy(i):
            slot = lax.rem(i, 2)
            return [pltpu.make_async_copy(o_v.at[slot], out_hbm.at[rows(i * ta, ta), :], sem_o.at[slot])]

        def w_copy(k):
            return [pltpu.make_async_copy((wg_hbm, wu_hbm)[k], (wg_v, wu_v)[k], sem_w.at[k])]

        def dd_copies(k):
            far = [
                send(
                    dwd_hbm.at[rows((2 * m + 1 - core) * own_d + k * rd, rd), :],
                    bd_v.at[k, m],
                    (dd.at[0, k, m], dd.at[1, k, m]),
                    partner,
                )
                for m in range(2)
            ]
            near = [
                pltpu.make_async_copy(dwd_hbm.at[rows((2 * m + core) * own_d + k * rd, rd), :], own_v.at[k, m], dl.at[0, k, m])
                for m in range(2)
            ]
            return far + near

        def dx_copies(k):
            return [send(sx_v.at[k], bx_v.at[k], (dx.at[0, k], dx.at[1, k]), across)]

        def dr_copies(k):
            return [
                send(sx_v.at[k, :, rows(n * qd, qd, 128)], br_v.at[k, m], (dr.at[0, k, m], dr.at[1, k, m]), to)
                for m, (n, to) in enumerate(peers)
            ]

        def dg_copies(k):
            at = (rows(k * rd, rd), rows(me_r * qd, qd, 128))
            far = [send(sg_v.at[k], od_hbm.at[at], (dg.at[0, k, m], dg.at[1, k, m]), to) for m, (_, to) in enumerate(peers)]
            return far + [pltpu.make_async_copy(sg_v.at[k], od_hbm.at[at], dl.at[1, k, 0])]

        def f0(k):
            start(dd_copies(k))

        def f1(k):
            wait(dd_copies(k))
            ac_v[k] = own_v[k, x].astype(F32) + bd_v[k, x].astype(F32)
            sx_v[k] = (own_v[k, 1 - x].astype(F32) + bd_v[k, 1 - x].astype(F32)).astype(BF)
            start(dx_copies(k))

        def f2(k):
            wait(dx_copies(k))
            total = ac_v[k] + bx_v[k].astype(F32)
            ac_v[k] = total
            sx_v[k] = total.astype(BF)
            start(dr_copies(k))

        def f3(k):
            wait(dr_copies(k))
            total = ac_v[k, :, rows(me_r * qd, qd, 128)]
            for m in range(3):
                total = total + br_v[k, m].astype(F32)
            sg_v[k] = total.astype(BF)
            start(dg_copies(k))

        def f4(k):
            wait(dg_copies(k))

        end = CHUNKS - 1
        todo = {
            0: [lambda: e4(end - 2), lambda: e2(end - 1, False, False), lambda: e0(end, False)],
            1: [lambda: e1(end, False, True)],
            2: [lambda: f1(0), lambda: f1(1)],
            3: [lambda: e3(end - 1, False), lambda: f1(2)],
            4: [lambda: f1(3), lambda: f1(4)],
            5: [lambda: e2(end, False, True)],
            6: [lambda: e4(end - 1)],
            7: [lambda: f2(0)],
            8: [lambda: e3(end, True)],
            9: [lambda: f2(1), lambda: f3(0)],
            11: [lambda: f2(2), lambda: f3(1)],
            12: [lambda: e4(end)],
            13: [lambda: f2(3), lambda: f3(2)],
            15: [lambda: f2(4), lambda: f3(3)],
        }

        def events(i, half):
            for point, does in todo.items():
                if point % 2 == half:

                    @pl.when(i == point // 2)
                    def _(does=does):
                        for do in does:
                            do()

        start(w_copy(0))
        start(i_copies(0))
        start(w_copy(1))
        for p in everyone:
            pl.semaphore_signal(entered, inc=1, device_id=p, device_id_type=MESH)
        pl.semaphore_wait(entered, 5)
        for k in range(5):
            f0(k)

        def tile(i, _):
            slot = lax.rem(i, 2)

            @pl.when(i + 1 < 8)
            def _():
                start(i_copies(i + 1))

            events(i, 0)
            wait(i_copies(i))

            @pl.when(i == 0)
            def _():
                wait(w_copy(0))

            by_g = dot(dgu_v[slot, :, pl.ds(0, f)], wg_v[...], NT).astype(BF)
            o_v[slot] = by_g
            events(i, 1)

            @pl.when(i == 0)
            def _():
                wait(w_copy(1))

            by_u = dot(dgu_v[slot, :, pl.ds(f, f)], wu_v[...], NT).astype(BF)
            by_a = (o_v[slot].astype(F32) + by_u.astype(F32)).astype(BF).astype(F32)
            wide = h_v[slot].astype(F32)
            scale = scale_of(wide)
            by_scale = jnp.sum(by_a * wide, -1, keepdims=True)
            by_wide = (by_a * scale - (by_scale * scale * scale * scale * (1.0 / d)) * wide).astype(BF)
            o_v[slot] = (dy_v[slot].astype(F32) + by_wide.astype(F32)).astype(BF)
            start(o_copy(i))

            @pl.when(i >= 1)
            def _():
                wait(o_copy(i - 1))

            return 0

        lax.fori_loop(0, 8, tile, 0)
        wait(o_copy(7))
        f3(4)
        for k in range(5):
            f4(k)

    pl.run_scoped(
        last,
        pltpu.VMEM((d, f), BF),
        pltpu.VMEM((d, f), BF),
        pltpu.VMEM((2, ta, 2 * f), BF),
        pltpu.VMEM((2, ta, d), BF),
        pltpu.VMEM((2, ta, d), BF),
        pltpu.VMEM((2, ta, d), BF),
        pltpu.VMEM((5, 2, rd, d), BF),
        pltpu.VMEM((5, 2, rd, d), BF),
        pltpu.VMEM((5, rd, d), F32),
        pltpu.VMEM((5, rd, d), BF),
        pltpu.VMEM((5, rd, d), BF),
        pltpu.VMEM((5, 3, rd, qd), BF),
        pltpu.VMEM((5, rd, qd), BF),
        pltpu.SemaphoreType.DMA((2,)),
        pltpu.SemaphoreType.DMA((2, 3)),
        pltpu.SemaphoreType.DMA((2,)),
        pltpu.SemaphoreType.DMA((2, 5, 2)),
        pltpu.SemaphoreType.DMA((2, 5)),
        pltpu.SemaphoreType.DMA((2, 5, 3)),
        pltpu.SemaphoreType.DMA((2, 5, 3)),
        pltpu.SemaphoreType.DMA((2, 5, 2)),
    )


def backward(a, h, dy, wg, wu, wd, saved, number):
    t, d = a.shape
    f = wd.shape[0]
    c = f // CHUNKS
    own, dma = d // 4, pltpu.SemaphoreType.DMA
    shapes = [(t, d), (own, f), (own, f), (f // 4, d), (t, 2 * f), (f, d)]
    out = pl.pallas_call(
        functools.partial(backward_kernel, saved is not None),
        in_specs=[ANY] * (8 if saved is not None else 6),
        out_specs=[ANY] * len(shapes),
        out_shape=[jax.ShapeDtypeStruct(s, BF) for s in shapes],
        scratch_shapes=[
            pltpu.VMEM((d, 2 * c), BF),
            pltpu.VMEM((2, own, 2 * c), BF),
            pltpu.VMEM((2, own, 2 * c), F32),
            pltpu.VMEM((own, 2 * c), BF),
            pltpu.VMEM((own, 2 * c), BF),
            pltpu.VMEM((own, 2 * c), BF),
            pltpu.VMEM((3, own // 4, 2 * c), BF),
            pltpu.VMEM((own // 4, 2 * c), BF),
            dma((2, 2)),
            dma((2,)),
            dma((2, 3)),
            dma((2, 2, 2, 3)),
            dma((2,)),
            pltpu.SemaphoreType.REGULAR,
            pltpu.SemaphoreType.REGULAR,
            pltpu.SemaphoreType.REGULAR((3,)),
            pltpu.SemaphoreType.REGULAR,
        ],
        compiler_params=pltpu.CompilerParams(vmem_limit_bytes=VMEM_LIMIT, collective_id=number, has_side_effects=True),
        cost_estimate=pl.CostEstimate(
            flops=(12 if saved is not None else 16) * t * d * f, bytes_accessed=30 * t * f, transcendentals=t * f
        ),
        name=f"backward_{number}",
    )(a, h, dy, wg, wu, wd, *(saved or ()))
    return out[:4]


def solution(mesh):
    def step(x, dy, *weights):
        def fetched(number):
            return [lax.all_gather(w[number], "s", axis=0, tiled=True) for w in weights]

        x, dy = x[0], dy[0]
        wg, wu, wd = fetched(0)
        a0, hid, g, u = gate_up(x, wg, wu)
        h, a1 = down(hid, wd, x)
        by_h, *top = backward(a1, h, dy, *fetched(1), None, 1)
        by_x, *bottom = backward(a0, x, by_h, wg, wu, wd, (g, u), 0)
        return (by_x[None], *(jnp.stack(pair) for pair in zip(bottom, top, strict=True)))

    states, cut = P(("rep", "r", "s"), None, None), P(None, "s", None)
    return jax.shard_map(
        step,
        mesh=mesh,
        in_specs=(states, states) + (cut,) * 3,
        out_specs=(states,) + (P("rep", "s", None),) * 3,
        check_vma=False,
    )
```

```python
import functools

import jax
import jax.numpy as jnp
from jax import lax
from jax.experimental import pallas as pl
from jax.experimental.pallas import tpu as pltpu
from jax.sharding import PartitionSpec as P

BF, F32 = jnp.bfloat16, jnp.float32
MESH = pl.DeviceIdType.MESH
NT = (((1,), (1,)), ((), ()))
TN = (((0,), (0,)), ((), ()))
ANY = pl.BlockSpec(memory_space=pl.ANY)
CHUNKS = 5
VMEM_LIMIT = 67043328


def dot(a, b, dims=(((1,), (0,)), ((), ()))):
    return lax.dot_general(a, b, dims, preferred_element_type=F32)


def scale_of(wide):
    return lax.rsqrt(jnp.mean(wide * wide, -1, keepdims=True) + 1e-6)


def pieces(width):
    first = 256 if width > 512 else width // 2
    return ((0, first), (first, width - first))


def rows(start, size, unit=16):
    return pl.ds(pl.multiple_of(start, unit) if size % unit == 0 else start, size)


def here():
    s = lax.axis_index("s")
    return lax.axis_index("r"), lax.div(s, 2), lax.rem(s, 2)


def send(src, dst, sems, to):
    return pltpu.make_async_remote_copy(
        src_ref=src, dst_ref=dst, send_sem=sems[0], recv_sem=sems[1], device_id=to, device_id_type=MESH
    )


def start(copies):
    for copy in copies:
        copy.start()


def wait(copies):
    for copy in copies:
        copy.wait()


def guarded(condition, do):
    @pl.when(condition)
    def _():
        do()


def neighbours():
    me_r, x, core = here()
    partner = {"s": x * 2 + (1 - core)}
    across = {"s": (1 - x) * 2 + core}
    peers = [(lax.rem(me_r + k, 4), {"r": lax.rem(me_r + k, 4)}) for k in (1, 2, 3)]
    return partner, across, peers


def meet(everyone):
    barrier = pltpu.get_barrier_semaphore()
    for p in everyone:
        pl.semaphore_signal(barrier, inc=1, device_id=p, device_id_type=MESH)
    pl.semaphore_wait(barrier, len(everyone))


def forward_kernel(x_hbm, wg_own, wu_own, wd_own, *refs):
    a_hbm, hid_hbm, g_hbm, u_hbm, h_hbm, a1_hbm, wg_all, wu_all, wd_all = refs[:9]
    (a_v, w_v, x_v, hid_v, g_v, u_v, wd_v, hi_v, xi_v, ho_v, ao_v, bg_v, bd_v) = refs[9:22]
    sem_x, sem_y, sem_d, sem_b, sem_w, sem_i, sem_ao, sem_o, sem_wd, sem_p, sem_q = refs[22:]
    t, d = x_hbm.shape
    f = hid_hbm.shape[1]
    c = f // CHUNKS
    me_r, x, core = here()
    me, oa = 2 * x + core, 2 * (1 - x) + core
    partner, across, peers = neighbours()
    meet([partner, across] + [p for _, p in peers])

    p0 = pieces(c)[0][1]
    runs = [(0, p0), (p0, c - p0)] + [(c * k, c) for k in range(1, CHUNKS)]

    class Piece:
        def __init__(self, number, layer, own, full, lo, width):
            self.n = number
            held = own.shape[1]
            unit = 16 if held % 16 == 0 and held >= 128 else 4
            self.q = held * 3 // 16 // unit * unit
            self.direct = held - 4 * self.q
            self.held = held
            self.own = lambda at, size: own.at[layer, rows(at, size), pl.ds(lo, width)]
            self.full = lambda at, size: full.at[layer, rows(at, size), pl.ds(lo, width)]

        def quarter(self):
            at, to = self.direct + me_r * self.q, me * self.held
            return send(self.own(at, self.q), self.full(to + at, self.q), (sem_x.at[0, self.n, 0], sem_x.at[1, self.n, 0]), across)

        def straight(self):
            sems = (sem_x.at[0, self.n, 1], sem_x.at[1, self.n, 1])
            return send(self.own(0, self.direct), self.full(me * self.held, self.direct), sems, across)

        def y_copies(self):
            block = self.full(oa * self.held + self.direct + me_r * self.q, self.q)
            return [send(block, block, (sem_y.at[0, self.n, k], sem_y.at[1, self.n, k]), to) for k, (_, to) in enumerate(peers)]

        def mine(self):
            sems = (sem_d.at[0, self.n, 0], sem_d.at[1, self.n, 0])
            return send(self.own(0, self.held), self.full(me * self.held, self.held), sems, partner)

        def theirs(self):
            block = self.full(oa * self.held, self.held)
            return send(block, block, (sem_d.at[0, self.n, 1], sem_d.at[1, self.n, 1]), partner)

    gate_up = [
        [Piece(2 * p + m, 0, own, full, lo, width) for m, (own, full) in enumerate(((wg_own, wg_all), (wu_own, wu_all)))]
        for p, (lo, width) in enumerate(runs)
    ]
    n = 2 * len(runs)
    d0, g1, u1, d1 = (
        [Piece(n, 0, wd_own, wd_all, 0, d)],
        [Piece(n + 1, 1, wg_own, wg_all, 0, f)],
        [Piece(n + 2, 1, wu_own, wu_all, 0, f)],
        [Piece(n + 3, 1, wd_own, wd_all, 0, d)],
    )

    def h0(group):
        for p in group:
            p.quarter().start()
            p.straight().start()
        for p in group:
            p.mine().start()

    def h1(group):
        for p in group:
            p.quarter().wait()
            start(p.y_copies())

    def h2(group):
        for p in group:
            p.straight().wait()
            wait(p.y_copies())
            p.theirs().start()

    def h3(group):
        for p in group:
            p.mine().wait()
            p.theirs().wait()

    blocks = [(wg_own, wg_all, bg_v), (wu_own, wu_all, bg_v), (wd_own, wd_all, bd_v)]

    def b_in(layer, m):
        own, _, via = blocks[m]
        return pltpu.make_async_copy(own.at[layer], via, sem_b.at[m // 2, 0])

    def b_out(layer, m):
        own, full, via = blocks[m]
        return pltpu.make_async_copy(via, full.at[layer, rows(me * own.shape[1], own.shape[1]), :], sem_b.at[m // 2, 1])

    def b0(layer, m):
        b_in(layer, m).start()

    def b1(layer, m):
        b_in(layer, m).wait()
        b_out(layer, m).start()

    def b2(layer, m):
        b_out(layer, m).wait()

    def load(k):
        lo, width = runs[k]
        at = pl.ds(lo, width)
        return [
            pltpu.make_async_copy(full.at[0, :, at], w_v.at[k % 2, :, pl.ds(m * c, width)], sem_w.at[k % 2, m])
            for m, full in enumerate((wg_all, wu_all))
        ]

    def load_d():
        return [pltpu.make_async_copy(wd_all.at[0], wd_v, sem_wd)]

    h0(gate_up[0])
    h0(gate_up[1])
    b0(0, 0)
    b0(0, 2)

    tm = t // 4

    def x_copy(i):
        return [pltpu.make_async_copy(x_hbm.at[rows(i * tm, tm), :], x_v.at[i % 2], sem_i.at[i % 2])]

    def a_copy(i):
        return [pltpu.make_async_copy(a_v.at[rows(i * tm, tm), :], a_hbm.at[rows(i * tm, tm), :], sem_ao.at[i])]

    start(x_copy(0))
    h0(gate_up[2])
    for i in range(4):
        if i < 3:
            start(x_copy(i + 1))
        wait(x_copy(i))

        def norm(k, _, i=i):
            at = rows(k * (tm // 4), tm // 4)
            wide = x_v[i % 2, at, :].astype(F32)
            a_v[rows(i * tm + k * (tm // 4), tm // 4), :] = (wide * scale_of(wide)).astype(BF)
            return 0

        lax.fori_loop(0, 4, norm, 0)
        start(a_copy(i))
        if i == 0:
            b1(0, 0)
            b1(0, 2)
        if i == 1:
            b2(0, 0)
            b0(0, 1)
            h1(gate_up[0])
        if i == 2:
            b1(0, 1)
            h0(gate_up[3])
    h1(gate_up[1])
    h2(gate_up[0])
    b2(0, 1)
    h3(gate_up[0])
    start(load(0))

    def o_copies(slot, i, lo, width):
        at = (rows(i * tm, tm), rows(lo, width, 128))
        near = pl.ds(0, width)
        return [
            pltpu.make_async_copy(v.at[slot, :, near], o.at[at], sem_o.at[slot, m])
            for m, (v, o) in enumerate(((hid_v, hid_hbm), (g_v, g_hbm), (u_v, u_hbm)))
        ]

    def compute(i, lo, width, parts, w_slot):
        slot = lax.rem(i, 2)
        a = a_v[rows(i * tm, tm), :]
        for at, w in parts:
            both = dot(a, jnp.concatenate([w_v[w_slot, :, pl.ds(at, w)], w_v[w_slot, :, pl.ds(c + at, w)]], 1))
            g, u = both[:, :w], both[:, w:]
            g_v[slot, :, pl.ds(at, w)] = g
            u_v[slot, :, pl.ds(at, w)] = u
            hid_v[slot, :, pl.ds(at, w)] = (g * jax.nn.sigmoid(g) * u).astype(BF)
        start(o_copies(slot, i, lo, width))

    td = t // 8

    def i_copies(m):
        at = rows(m * td, td)
        return [
            pltpu.make_async_copy(hid_hbm.at[at, :], hi_v.at[lax.rem(m, 2)], sem_p.at[lax.rem(m, 2), 0]),
            pltpu.make_async_copy(x_hbm.at[at, :], xi_v.at[lax.rem(m, 2)], sem_p.at[lax.rem(m, 2), 1]),
        ]

    def q_copies(m):
        at = rows(m * td, td)
        return [
            pltpu.make_async_copy(ho_v.at[lax.rem(m, 2)], h_hbm.at[at, :], sem_q.at[lax.rem(m, 2), 0]),
            pltpu.make_async_copy(ao_v.at[lax.rem(m, 2)], a1_hbm.at[at, :], sem_q.at[lax.rem(m, 2), 1]),
        ]

    gu = gate_up
    before = {
        (0, 1): lambda: (b0(1, 0), b2(0, 2), b0(1, 2)),
        (0, 2): lambda: (h2(gu[1]), h1(gu[2])),
        (0, 3): lambda: (h3(gu[1]), start(load(1)), h0(gu[4])),
        (1, 1): lambda: (b1(1, 0), b1(1, 2)),
        (1, 2): lambda: h1(gu[3]),
        (1, 3): lambda: (h2(gu[2]), b2(1, 0), b0(1, 1), b2(1, 2)),
        (2, -1): lambda: (h3(gu[2]), start(load(2)), h0(gu[5])),
        (2, 0): lambda: (h1(gu[4]), b1(1, 1)),
        (2, 1): lambda: (h2(gu[3]), h0(d0)),
        (2, 2): lambda: (h1(gu[5]), h3(gu[3]), start(load(3))),
        (2, 3): lambda: (h2(gu[4]), h0(g1), b2(1, 1)),
        (3, 1): lambda: (h2(gu[5]), h3(gu[4])),
        (3, 3): lambda: (h1(d0), h3(gu[5]), h0(u1)),
        (4, -1): lambda: start(load(4)),
        (4, 1): lambda: h0(d1),
        (5, -1): lambda: start(load(5)),
        (5, 0): lambda: h1(g1),
        (5, 1): lambda: h2(d0),
        (5, 3): lambda: (h3(d0), start(load_d()), start(i_copies(0))),
    }
    def at_point(k, i):
        for (k0, i0), do in before.items():
            if isinstance(k, int):
                if k0 == k and i0 >= 0:
                    guarded(i == i0, do)
            elif k0 > 1 and (i0 < 0) == (i is None):
                guarded(k == k0 if i is None else jnp.logical_and(k == k0, i == i0), do)

    for k in (0, 1):
        lo, width = runs[k]
        first = max(width // 2 // 128 * 128, width // 2 if width < 256 else 0)
        wait(load(k))

        def tile(i, _, k=k, lo=lo, width=width, first=first):
            at_point(k, i)
            slot = lax.rem(i, 2)

            @pl.when(i >= 2)
            def _():
                wait(o_copies(slot, i - 2, lo, width))

            if k == 1:

                @pl.when(i < 2)
                def _():
                    wait(o_copies(slot, i + 2, *runs[0]))

            compute(i, lo, width, ((0, first), (first, width - first)), k)
            return 0

        lax.fori_loop(0, 4, tile, 0)

    def run(k, _):
        lo = (k - 1) * c
        w_slot = lax.rem(k, 2)
        at_point(k, None)
        for k0 in range(2, len(runs)):

            @pl.when(k == k0)
            def _(k0=k0):
                wait(load(k0))

        def tile(i, _):
            at_point(k, i)
            slot = lax.rem(i, 2)

            @pl.when(i >= 2)
            def _():
                wait(o_copies(slot, i - 2, lo, c))

            @pl.when(jnp.logical_and(i < 2, k == 2))
            def _():
                wait(o_copies(slot, i + 2, *runs[1]))

            @pl.when(jnp.logical_and(i < 2, k > 2))
            def _():
                wait(o_copies(slot, i + 2, lo - c, c))

            compute(i, lo, c, pieces(c), w_slot)
            return 0

        lax.fori_loop(0, 4, tile, 0)
        return 0

    lax.fori_loop(2, len(runs), run, 0)
    last = len(runs) - 1
    wait(o_copies(0, 2, *runs[last]))
    wait(o_copies(1, 3, *runs[last]))
    wait(load_d())
    before = {
        0: lambda: h1(u1),
        1: lambda: h2(g1),
        3: lambda: h3(g1),
        4: lambda: h1(d1),
        5: lambda: h2(u1),
        7: lambda: h3(u1),
    }

    def tile(m, _):
        slot = lax.rem(m, 2)

        @pl.when(m < 7)
        def _():
            start(i_copies(m + 1))

        for m0, do in before.items():
            guarded(m == m0, do)
        wait(i_copies(m))

        @pl.when(m > 1)
        def _():
            wait(q_copies(m - 2))

        h = (xi_v[slot].astype(F32) + dot(hi_v[slot], wd_v[...]).astype(BF).astype(F32)).astype(BF)
        ho_v[slot] = h
        wide = h.astype(F32)
        ao_v[slot] = (wide * scale_of(wide)).astype(BF)
        start(q_copies(m))
        return 0

    lax.fori_loop(0, 8, tile, 0)
    h2(d1)
    wait(q_copies(6))
    wait(q_copies(7))
    for i in range(4):
        wait(a_copy(i))
    h3(d1)


def forward(x, wg, wu, wd):
    t, d = x.shape
    f = wg.shape[2]
    c = f // CHUNKS
    n, dma = 2 * CHUNKS + 6, pltpu.SemaphoreType.DMA
    shapes = [((t, d), BF), ((t, f), BF), ((t, f), F32), ((t, f), F32), ((t, d), BF), ((t, d), BF)]
    shapes += [((2, d, f), BF), ((2, d, f), BF), ((2, f, d), BF)]
    return pl.pallas_call(
        forward_kernel,
        in_specs=[ANY] * 4,
        out_specs=[ANY] * len(shapes),
        out_shape=[jax.ShapeDtypeStruct(*s) for s in shapes],
        scratch_shapes=[
            pltpu.VMEM((t, d), BF),
            pltpu.VMEM((2, d, 2 * c), BF),
            pltpu.VMEM((2, t // 4, d), BF),
            pltpu.VMEM((2, t // 4, c), BF),
            pltpu.VMEM((2, t // 4, c), F32),
            pltpu.VMEM((2, t // 4, c), F32),
            pltpu.VMEM((f, d), BF),
            pltpu.VMEM((2, t // 8, f), BF),
            pltpu.VMEM((2, t // 8, d), BF),
            pltpu.VMEM((2, t // 8, d), BF),
            pltpu.VMEM((2, t // 8, d), BF),
            pltpu.VMEM(wg.shape[1:], BF),
            pltpu.VMEM(wd.shape[1:], BF),
            dma((2, n, 2)),
            dma((2, n, 3)),
            dma((2, n, 2)),
            dma((2, 2)),
            dma((2, 2)),
            dma((2,)),
            dma((4,)),
            dma((2, 3)),
            dma,
            dma((2, 2)),
            dma((2, 2)),
        ],
        compiler_params=pltpu.CompilerParams(vmem_limit_bytes=VMEM_LIMIT, collective_id=2, has_side_effects=True),
        cost_estimate=pl.CostEstimate(flops=6 * t * d * f, bytes_accessed=16 * t * f, transcendentals=t * f),
        name="forward",
    )(x, wg, wu, wd)


def backward_kernel(layer, *refs):
    saved = layer == 0
    n_in = 8 if saved else 6
    a_hbm, h_hbm, dy_hbm, wg_hbm, wu_hbm, wd_hbm = refs[:6]
    g_hbm, u_hbm = refs[6:n_in] if saved else (None, None)
    out_hbm, og_hbm, ou_hbm, od_hbm, dgu_hbm, dwd_hbm = refs[n_in : n_in + 6]
    (stg, buf_d, acc, buf_x, s_x, s_r, buf_r, s_g, sem_d, sem_x, sem_r, sem_g, sem_gl, free_d, free_x, free_r, entered) = refs[n_in + 6 :]

    t, d = a_hbm.shape
    f = wd_hbm.shape[1]
    c = f // CHUNKS
    own = d // 4
    quarter = own // 4
    own_d = f // 4
    rd = own_d // 5
    qd = d // 4
    me_r, x, core = here()
    partner, across, peers = neighbours()
    everyone = [partner, across] + [p for _, p in peers]
    meet(everyone)

    def d_copies():
        return [
            send(stg.at[rows((2 * k + 1 - core) * own, own), :], buf_d.at[k], (sem_d.at[0, k], sem_d.at[1, k]), partner)
            for k in range(2)
        ]

    def x_copies():
        return [send(s_x, buf_x, (sem_x.at[0], sem_x.at[1]), across)]

    def r_copies():
        return [
            send(s_r.at[rows(n * quarter, quarter), :], buf_r.at[k], (sem_r.at[0, k], sem_r.at[1, k]), p)
            for k, (n, p) in enumerate(peers)
        ]

    def g_copies(p):
        at = (rows(me_r * quarter, quarter), rows(p * c, c, 128))
        far = [
            send(s_g.at[:, pl.ds(i * c, c)], o.at[at], (sem_g.at[0, lax.rem(p, 2), i, k], sem_g.at[1, lax.rem(p, 2), i, k]), to)
            for k, (_, to) in enumerate(peers)
            for i, o in enumerate((og_hbm, ou_hbm))
        ]
        near = [pltpu.make_async_copy(s_g.at[:, pl.ds(i * c, c)], o.at[at], sem_gl.at[i]) for i, o in enumerate((og_hbm, ou_hbm))]
        return far + near

    def e0(p, first):
        if not first:
            pl.semaphore_wait(free_d, 1)
        start(d_copies())

    def e1(p, first, last):
        wait(d_copies())
        acc[lax.rem(p, 2)] = stg[rows((2 * x + core) * own, own), :].astype(F32) + buf_d[x].astype(F32)
        s_x[...] = (stg[rows((2 * (1 - x) + core) * own, own), :].astype(F32) + buf_d[1 - x].astype(F32)).astype(BF)
        if not last:
            pl.semaphore_signal(free_d, inc=1, device_id=partner, device_id_type=MESH)
        if not first:
            pl.semaphore_wait(free_x, 1)
        start(x_copies())

    def e2(p, first, last):
        wait(x_copies())
        total = acc[lax.rem(p, 2)] + buf_x[...].astype(F32)
        acc[lax.rem(p, 2)] = total
        s_r[...] = total.astype(BF)
        if not last:
            pl.semaphore_signal(free_x, inc=1, device_id=across, device_id_type=MESH)
        if not first:
            for k in range(3):
                pl.semaphore_wait(free_r.at[k], 1)
        start(r_copies())

    def e3(p, last):
        wait(r_copies())
        total = acc[lax.rem(p, 2), rows(me_r * quarter, quarter), :]
        for k in range(3):
            total = total + buf_r[k].astype(F32)
        s_g[...] = total.astype(BF)
        if not last:
            for k, (_, to) in enumerate(peers):
                pl.semaphore_signal(free_r.at[2 - k], inc=1, device_id=to, device_id_type=MESH)
        start(g_copies(p))

    def e4(p):
        wait(g_copies(p))

    tm = t // 8 if saved else t // 4
    tiles = t // tm

    def chunks(*bufs):
        if saved:
            a_v, dy_v, wd_v, hid_v, dgs, dst, g_v, u_v, sem_a, sem_w, sem_o, sem_s = bufs
        else:
            a_v, dy_v, wd_v, hid_v, dgs, dst, wgu_v, sem_a, sem_w, sem_o = bufs

        def a_copies(i):
            at = rows(i * tm, tm)
            return [
                pltpu.make_async_copy(a_hbm.at[at, :], a_v.at[at, :], sem_a.at[0, i]),
                pltpu.make_async_copy(dy_hbm.at[at, :], dy_v.at[at, :], sem_a.at[1, i]),
            ]

        def w_copies(j):
            slot = lax.rem(j, 2)
            at = rows(j * c, c, 128)
            w = [pltpu.make_async_copy(wd_hbm.at[layer, at, :], wd_v.at[slot], sem_w.at[slot, 0])]
            if not saved:
                w.append(pltpu.make_async_copy(wg_hbm.at[layer, :, at], wgu_v.at[slot, :, pl.ds(0, c)], sem_w.at[slot, 1]))
                w.append(pltpu.make_async_copy(wu_hbm.at[layer, :, at], wgu_v.at[slot, :, pl.ds(c, c)], sem_w.at[slot, 2]))
            return w

        def s_copies(n):
            slot = lax.rem(n, 2)
            at = (rows(lax.rem(n, tiles) * tm, tm), rows(lax.div(n, tiles) * c, c, 128))
            return [
                pltpu.make_async_copy(g_hbm.at[at], g_v.at[slot], sem_s.at[slot, 0]),
                pltpu.make_async_copy(u_hbm.at[at], u_v.at[slot], sem_s.at[slot, 1]),
            ]

        def o_copies(j):
            return [
                pltpu.make_async_copy(dgs.at[:, pl.ds(0, c)], dgu_hbm.at[:, rows(j * c, c, 128)], sem_o.at[0]),
                pltpu.make_async_copy(dgs.at[:, pl.ds(c, c)], dgu_hbm.at[:, rows(f + j * c, c, 128)], sem_o.at[1]),
            ]

        def dw_copy(j):
            return [pltpu.make_async_copy(dst, dwd_hbm.at[rows(j * c, c), :], sem_o.at[2])]

        start(w_copies(0))
        if saved:
            start(s_copies(0))
        for i in range(tiles):
            start(a_copies(i))

        def chunk(j, _):
            slot = lax.rem(j, 2)

            @pl.when(j >= 3)
            def _():
                e4(j - 3)

            @pl.when(j == 2)
            def _():
                e2(j - 2, True, False)

            @pl.when(j >= 3)
            def _():
                e2(j - 2, False, False)

            @pl.when(j == 1)
            def _():
                e0(j - 1, True)

            @pl.when(j >= 2)
            def _():
                e0(j - 1, False)

            @pl.when(j >= 1)
            def _():
                wait(o_copies(j - 1))

            wait(w_copies(j))

            @pl.when(j + 1 < CHUNKS)
            def _():
                start(w_copies(j + 1))

            def tile(i, _):
                @pl.when(j == 0)
                def _():
                    wait(a_copies(i))

                if saved:
                    n = j * tiles + i

                    @pl.when(n + 1 < CHUNKS * tiles)
                    def _():
                        start(s_copies(n + 1))

                    wait(s_copies(n))

                @pl.when(jnp.logical_and(i == tiles // 2, j == 1))
                def _():
                    e1(j - 1, True, False)

                @pl.when(jnp.logical_and(i == tiles // 2, j >= 2))
                def _():
                    e1(j - 1, False, False)

                r = rows(i * tm, tm)
                for p0, w in pieces(c):
                    if saved:
                        g = g_v[lax.rem(n, 2), :, pl.ds(p0, w)]
                        u = u_v[lax.rem(n, 2), :, pl.ds(p0, w)]
                    else:
                        a = a_v[r, :]
                        both = dot(a, jnp.concatenate([wgu_v[slot, :, pl.ds(p0, w)], wgu_v[slot, :, pl.ds(c + p0, w)]], 1))
                        g, u = both[:, :w], both[:, w:]
                    dh = dot(dy_v[r, :], wd_v[slot, pl.ds(p0, w), :], NT).astype(BF).astype(F32)
                    s = jax.nn.sigmoid(g)
                    silu = g * s
                    hid_v[r, pl.ds(p0, w)] = (silu * u).astype(BF)
                    dgs[r, pl.ds(c + p0, w)] = (dh * silu).astype(BF)
                    dgs[r, pl.ds(p0, w)] = (dh * u * (s + silu * (1.0 - s))).astype(BF)
                return 0

            lax.fori_loop(0, tiles, tile, 0)
            start(o_copies(j))

            @pl.when(j >= 1)
            def _():
                wait(dw_copy(j - 1))

            for p0, w in pieces(c):
                dst[pl.ds(p0, w), :] = dot(hid_v[:, pl.ds(p0, w)], dy_v[...], TN).astype(BF)
            start(dw_copy(j))

            @pl.when(j >= 2)
            def _():
                e3(j - 2, False)

            for k in range(2):
                stg[pl.ds(k * (d // 2), d // 2), :] = dot(a_v[:, pl.ds(k * (d // 2), d // 2)], dgs[...], TN).astype(BF)
            return 0

        lax.fori_loop(0, CHUNKS, chunk, 0)
        wait(o_copies(CHUNKS - 1))
        wait(dw_copy(CHUNKS - 1))

    bufs = [
        pltpu.VMEM((t, d), BF),
        pltpu.VMEM((t, d), BF),
        pltpu.VMEM((2, c, d), BF),
        pltpu.VMEM((t, c), BF),
        pltpu.VMEM((t, 2 * c), BF),
        pltpu.VMEM((c, d), BF),
    ]
    bufs += [pltpu.VMEM((2, tm, c), F32)] * 2 if saved else [pltpu.VMEM((2, d, 2 * c), BF)]
    bufs += [pltpu.SemaphoreType.DMA((2, tiles)), pltpu.SemaphoreType.DMA((2, 3)), pltpu.SemaphoreType.DMA((3,))]
    bufs += [pltpu.SemaphoreType.DMA((2, 2))] if saved else []
    pl.run_scoped(chunks, *bufs)

    ta = t // 8

    def last(wg_v, wu_v, dgu_v, h_v, dy_v, o_v, own_v, bd_v, ac_v, bx_v, sx_v, br_v, sg_v, sem_w, sem_i, sem_o, dd, dx, dr, dg, dl):
        def i_copies(i):
            slot = lax.rem(i, 2)
            at = rows(i * ta, ta)
            return [
                pltpu.make_async_copy(dgu_hbm.at[at, :], dgu_v.at[slot], sem_i.at[slot, 0]),
                pltpu.make_async_copy(h_hbm.at[at, :], h_v.at[slot], sem_i.at[slot, 1]),
                pltpu.make_async_copy(dy_hbm.at[at, :], dy_v.at[slot], sem_i.at[slot, 2]),
            ]

        def o_copy(i):
            slot = lax.rem(i, 2)
            return [pltpu.make_async_copy(o_v.at[slot], out_hbm.at[rows(i * ta, ta), :], sem_o.at[slot])]

        def w_copy(k):
            return [pltpu.make_async_copy((wg_hbm, wu_hbm)[k].at[layer], (wg_v, wu_v)[k], sem_w.at[k])]

        def dd_copies(k):
            far = [
                send(
                    dwd_hbm.at[rows((2 * m + 1 - core) * own_d + k * rd, rd), :],
                    bd_v.at[k, m],
                    (dd.at[0, k, m], dd.at[1, k, m]),
                    partner,
                )
                for m in range(2)
            ]
            near = [
                pltpu.make_async_copy(dwd_hbm.at[rows((2 * m + core) * own_d + k * rd, rd), :], own_v.at[k, m], dl.at[0, k, m])
                for m in range(2)
            ]
            return far + near

        def dx_copies(k):
            return [send(sx_v.at[k], bx_v.at[k], (dx.at[0, k], dx.at[1, k]), across)]

        def dr_copies(k):
            return [
                send(sx_v.at[k, :, rows(n * qd, qd, 128)], br_v.at[k, m], (dr.at[0, k, m], dr.at[1, k, m]), to)
                for m, (n, to) in enumerate(peers)
            ]

        def dg_copies(k):
            at = (rows(k * rd, rd), rows(me_r * qd, qd, 128))
            far = [send(sg_v.at[k], od_hbm.at[at], (dg.at[0, k, m], dg.at[1, k, m]), to) for m, (_, to) in enumerate(peers)]
            return far + [pltpu.make_async_copy(sg_v.at[k], od_hbm.at[at], dl.at[1, k, 0])]

        def f0(k):
            start(dd_copies(k))

        def f1(k):
            wait(dd_copies(k))
            ac_v[k] = own_v[k, x].astype(F32) + bd_v[k, x].astype(F32)
            sx_v[k] = (own_v[k, 1 - x].astype(F32) + bd_v[k, 1 - x].astype(F32)).astype(BF)
            start(dx_copies(k))

        def f2(k):
            wait(dx_copies(k))
            total = ac_v[k] + bx_v[k].astype(F32)
            ac_v[k] = total
            sx_v[k] = total.astype(BF)
            start(dr_copies(k))

        def f3(k):
            wait(dr_copies(k))
            total = ac_v[k, :, rows(me_r * qd, qd, 128)]
            for m in range(3):
                total = total + br_v[k, m].astype(F32)
            sg_v[k] = total.astype(BF)
            start(dg_copies(k))

        def f4(k):
            wait(dg_copies(k))

        end = CHUNKS - 1
        todo = {
            0: [lambda: e4(end - 2), lambda: e2(end - 1, False, False), lambda: e0(end, False)],
            1: [lambda: e1(end, False, True)],
            2: [lambda: f1(0), lambda: f1(1)],
            3: [lambda: e3(end - 1, False), lambda: f1(2)],
            4: [lambda: f1(3), lambda: f1(4)],
            5: [lambda: e2(end, False, True)],
            6: [lambda: e4(end - 1)],
            7: [lambda: f2(0)],
            8: [lambda: e3(end, True)],
            9: [lambda: f2(1), lambda: f3(0)],
            11: [lambda: f2(2), lambda: f3(1)],
            12: [lambda: e4(end)],
            13: [lambda: f2(3), lambda: f3(2)],
            15: [lambda: f2(4), lambda: f3(3)],
        }

        def events(i, half):
            for point, does in todo.items():
                if point % 2 == half:

                    @pl.when(i == point // 2)
                    def _(does=does):
                        for do in does:
                            do()

        start(w_copy(0))
        start(i_copies(0))
        start(w_copy(1))
        for p in everyone:
            pl.semaphore_signal(entered, inc=1, device_id=p, device_id_type=MESH)
        pl.semaphore_wait(entered, 5)
        for k in range(5):
            f0(k)

        def tile(i, _):
            slot = lax.rem(i, 2)

            @pl.when(i + 1 < 8)
            def _():
                start(i_copies(i + 1))

            events(i, 0)
            wait(i_copies(i))

            @pl.when(i == 0)
            def _():
                wait(w_copy(0))

            by_g = dot(dgu_v[slot, :, pl.ds(0, f)], wg_v[...], NT).astype(BF)
            o_v[slot] = by_g
            events(i, 1)

            @pl.when(i == 0)
            def _():
                wait(w_copy(1))

            by_u = dot(dgu_v[slot, :, pl.ds(f, f)], wu_v[...], NT).astype(BF)
            by_a = (o_v[slot].astype(F32) + by_u.astype(F32)).astype(BF).astype(F32)
            wide = h_v[slot].astype(F32)
            scale = scale_of(wide)
            by_scale = jnp.sum(by_a * wide, -1, keepdims=True)
            by_wide = (by_a * scale - (by_scale * scale * scale * scale * (1.0 / d)) * wide).astype(BF)
            o_v[slot] = (dy_v[slot].astype(F32) + by_wide.astype(F32)).astype(BF)
            start(o_copy(i))

            @pl.when(i >= 1)
            def _():
                wait(o_copy(i - 1))

            return 0

        lax.fori_loop(0, 8, tile, 0)
        wait(o_copy(7))
        f3(4)
        for k in range(5):
            f4(k)

    pl.run_scoped(
        last,
        pltpu.VMEM((d, f), BF),
        pltpu.VMEM((d, f), BF),
        pltpu.VMEM((2, ta, 2 * f), BF),
        pltpu.VMEM((2, ta, d), BF),
        pltpu.VMEM((2, ta, d), BF),
        pltpu.VMEM((2, ta, d), BF),
        pltpu.VMEM((5, 2, rd, d), BF),
        pltpu.VMEM((5, 2, rd, d), BF),
        pltpu.VMEM((5, rd, d), F32),
        pltpu.VMEM((5, rd, d), BF),
        pltpu.VMEM((5, rd, d), BF),
        pltpu.VMEM((5, 3, rd, qd), BF),
        pltpu.VMEM((5, rd, qd), BF),
        pltpu.SemaphoreType.DMA((2,)),
        pltpu.SemaphoreType.DMA((2, 3)),
        pltpu.SemaphoreType.DMA((2,)),
        pltpu.SemaphoreType.DMA((2, 5, 2)),
        pltpu.SemaphoreType.DMA((2, 5)),
        pltpu.SemaphoreType.DMA((2, 5, 3)),
        pltpu.SemaphoreType.DMA((2, 5, 3)),
        pltpu.SemaphoreType.DMA((2, 5, 2)),
    )


def backward(a, h, dy, wg, wu, wd, saved, layer):
    t, d = a.shape
    f = wd.shape[1]
    c = f // CHUNKS
    own, dma = d // 4, pltpu.SemaphoreType.DMA
    shapes = [(t, d), (own, f), (own, f), (f // 4, d), (t, 2 * f), (f, d)]
    out = pl.pallas_call(
        functools.partial(backward_kernel, layer),
        in_specs=[ANY] * (8 if saved is not None else 6),
        out_specs=[ANY] * len(shapes),
        out_shape=[jax.ShapeDtypeStruct(s, BF) for s in shapes],
        scratch_shapes=[
            pltpu.VMEM((d, 2 * c), BF),
            pltpu.VMEM((2, own, 2 * c), BF),
            pltpu.VMEM((2, own, 2 * c), F32),
            pltpu.VMEM((own, 2 * c), BF),
            pltpu.VMEM((own, 2 * c), BF),
            pltpu.VMEM((own, 2 * c), BF),
            pltpu.VMEM((3, own // 4, 2 * c), BF),
            pltpu.VMEM((own // 4, 2 * c), BF),
            dma((2, 2)),
            dma((2,)),
            dma((2, 3)),
            dma((2, 2, 2, 3)),
            dma((2,)),
            pltpu.SemaphoreType.REGULAR,
            pltpu.SemaphoreType.REGULAR,
            pltpu.SemaphoreType.REGULAR((3,)),
            pltpu.SemaphoreType.REGULAR,
        ],
        compiler_params=pltpu.CompilerParams(vmem_limit_bytes=VMEM_LIMIT, collective_id=layer, has_side_effects=True),
        cost_estimate=pl.CostEstimate(
            flops=(12 if saved is not None else 16) * t * d * f, bytes_accessed=30 * t * f, transcendentals=t * f
        ),
        name=f"backward_{layer}",
    )(a, h, dy, wg, wu, wd, *(saved or ()))
    return out[:4]


def solution(mesh):
    def step(x, dy, *weights):
        x, dy = x[0], dy[0]
        a0, _, g, u, h, a1, *whole = forward(x, *weights)
        by_h, *top = backward(a1, h, dy, *whole, None, 1)
        by_x, *bottom = backward(a0, x, by_h, *whole, (g, u), 0)
        return (by_x[None], *(jnp.stack(pair) for pair in zip(bottom, top, strict=True)))

    states, cut = P(("rep", "r", "s"), None, None), P(None, "s", None)
    return jax.shard_map(
        step,
        mesh=mesh,
        in_specs=(states, states) + (cut,) * 3,
        out_specs=(states,) + (P("rep", "s", None),) * 3,
        check_vma=False,
    )
```

```python
import functools

import jax
import jax.numpy as jnp
from jax import lax
from jax.experimental import pallas as pl
from jax.experimental.pallas import tpu as pltpu
from jax.sharding import PartitionSpec as P

BF, F32 = jnp.bfloat16, jnp.float32
MESH = pl.DeviceIdType.MESH
NT = (((1,), (1,)), ((), ()))
TN = (((0,), (0,)), ((), ()))
ANY = pl.BlockSpec(memory_space=pl.ANY)
CHUNKS = 5
VMEM_LIMIT = 67043328


def dot(a, b, dims=(((1,), (0,)), ((), ()))):
    return lax.dot_general(a, b, dims, preferred_element_type=F32)


def scale_of(wide):
    return lax.rsqrt(jnp.mean(wide * wide, -1, keepdims=True) + 1e-6)


def pieces(width):
    first = 256 if width > 512 else width // 2
    return ((0, first), (first, width - first))


def rows(start, size, unit=16):
    return pl.ds(pl.multiple_of(start, unit) if size % unit == 0 else start, size)


def here():
    s = lax.axis_index("s")
    return lax.axis_index("r"), lax.div(s, 2), lax.rem(s, 2)


def send(src, dst, sems, to):
    return pltpu.make_async_remote_copy(
        src_ref=src, dst_ref=dst, send_sem=sems[0], recv_sem=sems[1], device_id=to, device_id_type=MESH
    )


def start(copies):
    for copy in copies:
        copy.start()


def wait(copies):
    for copy in copies:
        copy.wait()


def guarded(condition, do):
    @pl.when(condition)
    def _():
        do()


def neighbours():
    me_r, x, core = here()
    partner = {"s": x * 2 + (1 - core)}
    across = {"s": (1 - x) * 2 + core}
    peers = [(lax.rem(me_r + k, 4), {"r": lax.rem(me_r + k, 4)}) for k in (1, 2, 3)]
    return partner, across, peers


def meet(everyone):
    barrier = pltpu.get_barrier_semaphore()
    for p in everyone:
        pl.semaphore_signal(barrier, inc=1, device_id=p, device_id_type=MESH)
    pl.semaphore_wait(barrier, len(everyone))


def forward_kernel(x_hbm, wg_own, wu_own, wd_own, *refs):
    a_hbm, hid_hbm, g_hbm, u_hbm, h_hbm, a1_hbm, wg_all, wu_all, wd_all = refs[:9]
    (a_v, w_v, x_v, hid_v, g_v, u_v, wd_v, hi_v, xi_v, ho_v, ao_v, bg_v, bd_v) = refs[9:22]
    sem_x, sem_y, sem_d, sem_b, sem_w, sem_i, sem_ao, sem_o, sem_wd, sem_p, sem_q = refs[22:]
    t, d = x_hbm.shape
    f = hid_hbm.shape[1]
    c = f // CHUNKS
    me_r, x, core = here()
    me, oa = 2 * x + core, 2 * (1 - x) + core
    partner, across, peers = neighbours()
    meet([partner, across] + [p for _, p in peers])

    p0 = pieces(c)[0][1]
    runs = [(0, p0), (p0, c - p0)] + [(c * k, c) for k in range(1, CHUNKS)]

    class Piece:
        def __init__(self, number, layer, own, full, lo, width):
            self.n = number
            held = own.shape[1]
            unit = 16 if held % 16 == 0 and held >= 128 else 4
            self.q = held * 3 // 16 // unit * unit
            self.direct = held - 4 * self.q
            self.held = held
            self.own = lambda at, size: own.at[layer, rows(at, size), pl.ds(lo, width)]
            self.full = lambda at, size: full.at[layer, rows(at, size), pl.ds(lo, width)]

        def quarter(self):
            at, to = self.direct + me_r * self.q, me * self.held
            return send(self.own(at, self.q), self.full(to + at, self.q), (sem_x.at[0, self.n, 0], sem_x.at[1, self.n, 0]), across)

        def straight(self):
            sems = (sem_x.at[0, self.n, 1], sem_x.at[1, self.n, 1])
            return send(self.own(0, self.direct), self.full(me * self.held, self.direct), sems, across)

        def y_copies(self):
            block = self.full(oa * self.held + self.direct + me_r * self.q, self.q)
            return [send(block, block, (sem_y.at[0, self.n, k], sem_y.at[1, self.n, k]), to) for k, (_, to) in enumerate(peers)]

        def mine(self):
            sems = (sem_d.at[0, self.n, 0], sem_d.at[1, self.n, 0])
            return send(self.own(0, self.held), self.full(me * self.held, self.held), sems, partner)

        def theirs(self):
            block = self.full(oa * self.held, self.held)
            return send(block, block, (sem_d.at[0, self.n, 1], sem_d.at[1, self.n, 1]), partner)

    gate_up = [
        [Piece(2 * p + m, 0, own, full, lo, width) for m, (own, full) in enumerate(((wg_own, wg_all), (wu_own, wu_all)))]
        for p, (lo, width) in enumerate(runs)
    ]
    n = 2 * len(runs)
    d0, g1, u1, d1 = (
        [Piece(n, 0, wd_own, wd_all, 0, d)],
        [Piece(n + 1, 1, wg_own, wg_all, 0, f)],
        [Piece(n + 2, 1, wu_own, wu_all, 0, f)],
        [Piece(n + 3, 1, wd_own, wd_all, 0, d)],
    )

    def h0(group):
        for p in group:
            p.quarter().start()
            p.straight().start()
        for p in group:
            p.mine().start()

    def h1(group):
        for p in group:
            p.quarter().wait()
            start(p.y_copies())

    def h2(group):
        for p in group:
            p.straight().wait()
            wait(p.y_copies())
            p.theirs().start()

    def h3(group):
        for p in group:
            p.mine().wait()
            p.theirs().wait()

    blocks = [(wg_own, wg_all, bg_v), (wu_own, wu_all, bg_v), (wd_own, wd_all, bd_v)]

    def b_in(layer, m):
        own, _, via = blocks[m]
        return pltpu.make_async_copy(own.at[layer], via, sem_b.at[m // 2, 0])

    def b_out(layer, m):
        own, full, via = blocks[m]
        return pltpu.make_async_copy(via, full.at[layer, rows(me * own.shape[1], own.shape[1]), :], sem_b.at[m // 2, 1])

    def b0(layer, m):
        b_in(layer, m).start()

    def b1(layer, m):
        b_in(layer, m).wait()
        b_out(layer, m).start()

    def b2(layer, m):
        b_out(layer, m).wait()

    def load(k):
        lo, width = runs[k]
        at = pl.ds(lo, width)
        return [
            pltpu.make_async_copy(full.at[0, :, at], w_v.at[k % 2, :, pl.ds(m * c, width)], sem_w.at[k % 2, m])
            for m, full in enumerate((wg_all, wu_all))
        ]

    def load_d():
        return [pltpu.make_async_copy(wd_all.at[0], wd_v, sem_wd)]

    h0(gate_up[0])
    h0(gate_up[1])

    tm = t // 4
    td = t // 8
    tn = min(64, td)

    def x_copy(i):
        return [pltpu.make_async_copy(x_hbm.at[rows(i * td, td), :], x_v.at[i % 4], sem_i.at[i % 4])]

    def a_copy(i):
        return [pltpu.make_async_copy(a_v.at[rows(i * td, td), :], a_hbm.at[rows(i * td, td), :], sem_ao.at[i])]

    for i in range(4):
        start(x_copy(i))
    b0(0, 0)
    b0(0, 2)
    h0(gate_up[2])
    for i in range(8):
        wait(x_copy(i))

        def norm(k, _, i=i):
            wide = x_v[i % 4, rows(k * tn, tn), :].astype(F32)
            a_v[rows(i * td + k * tn, tn), :] = (wide * scale_of(wide)).astype(BF)
            return 0

        lax.fori_loop(0, td // tn, norm, 0)
        start(a_copy(i))
        if i < 4:
            start(x_copy(i + 4))
        if i == 1:
            b1(0, 0)
            b1(0, 2)
        if i == 2:
            h1(gate_up[0])
            b2(0, 0)
            b0(0, 1)
        if i == 4:
            b1(0, 1)
            h1(gate_up[1])
        if i == 5:
            h2(gate_up[0])
            b2(0, 1)
            h0(gate_up[3])
    h3(gate_up[0])
    start(load(0))
    h0(gate_up[4])

    def o_copies(slot, i, lo, width):
        at = (rows(i * tm, tm), rows(lo, width, 128))
        near = pl.ds(0, width)
        return [
            pltpu.make_async_copy(v.at[slot, :, near], o.at[at], sem_o.at[slot, m])
            for m, (v, o) in enumerate(((hid_v, hid_hbm), (g_v, g_hbm), (u_v, u_hbm)))
        ]

    def compute(i, lo, width, parts, w_slot):
        slot = lax.rem(i, 2)
        a = a_v[rows(i * tm, tm), :]
        for at, w in parts:
            both = dot(a, jnp.concatenate([w_v[w_slot, :, pl.ds(at, w)], w_v[w_slot, :, pl.ds(c + at, w)]], 1))
            g, u = both[:, :w], both[:, w:]
            s = jax.nn.sigmoid(g)
            silu = g * s
            g_v[slot, :, pl.ds(at, w)] = u * (s + silu * (1.0 - s))
            u_v[slot, :, pl.ds(at, w)] = silu
            hid_v[slot, :, pl.ds(at, w)] = (silu * u).astype(BF)
        start(o_copies(slot, i, lo, width))

    def i_copies(m):
        at = rows(m * td, td)
        return [
            pltpu.make_async_copy(hid_hbm.at[at, :], hi_v.at[lax.rem(m, 2)], sem_p.at[lax.rem(m, 2), 0]),
            pltpu.make_async_copy(x_hbm.at[at, :], xi_v.at[lax.rem(m, 2)], sem_p.at[lax.rem(m, 2), 1]),
        ]

    def h_copy(m):
        return [pltpu.make_async_copy(ho_v.at[lax.rem(m, 2)], h_hbm.at[rows(m * td, td), :], sem_q.at[lax.rem(m, 2), 0])]

    def a1_copy(m):
        return [pltpu.make_async_copy(ao_v.at[lax.rem(m, 2)], a1_hbm.at[rows(m * td, td), :], sem_q.at[lax.rem(m, 2), 1])]

    gu = gate_up
    before = {
        (0, 1): lambda: (b0(1, 0), b2(0, 2), b0(1, 2)),
        (0, 2): lambda: (h2(gu[1]), h1(gu[2])),
        (0, 3): lambda: (h3(gu[1]), start(load(1)), h0(gu[5])),
        (1, 0): lambda: (b1(1, 0), b1(1, 2)),
        (1, 1): lambda: (h2(gu[2]), h1(gu[3]), h0(d0)),
        (1, 2): lambda: (h3(gu[2]), start(load(2))),
        (1, 3): lambda: (b2(1, 0), b0(1, 1), b2(1, 2)),
        (2, 0): lambda: (h2(gu[3]), h1(gu[4]), b1(1, 1), h0(g1)),
        (2, 1): lambda: (h3(gu[3]), start(load(3))),
        (2, 2): lambda: h1(gu[5]),
        (2, 3): lambda: (h2(gu[4]), b2(1, 1)),
        (3, 0): lambda: (h3(gu[4]), start(load(4)), h0(u1)),
        (3, 1): lambda: (h2(gu[5]), h1(d0)),
        (3, 2): lambda: h3(gu[5]),
        (4, 0): lambda: (start(load(5)), h0(d1)),
        (4, 2): lambda: (h2(d0), h1(g1)),
        (5, 0): lambda: (h3(d0), start(load_d())),
        (5, 2): lambda: (h2(g1), h1(u1)),
        (5, 3): lambda: start(i_copies(0)),
    }

    def at_point(k, i):
        for (k0, i0), do in before.items():
            if isinstance(k, int):
                if k0 == k and i0 >= 0:
                    guarded(i == i0, do)
            elif k0 > 1 and (i0 < 0) == (i is None):
                guarded(k == k0 if i is None else jnp.logical_and(k == k0, i == i0), do)

    for k in (0, 1):
        lo, width = runs[k]
        first = max(width // 2 // 128 * 128, width // 2 if width < 256 else 0)
        wait(load(k))

        def tile(i, _, k=k, lo=lo, width=width, first=first):
            at_point(k, i)
            slot = lax.rem(i, 2)

            @pl.when(i >= 2)
            def _():
                wait(o_copies(slot, i - 2, lo, width))

            if k == 1:

                @pl.when(i < 2)
                def _():
                    wait(o_copies(slot, i + 2, *runs[0]))

            compute(i, lo, width, ((0, first), (first, width - first)), k)
            return 0

        lax.fori_loop(0, 4, tile, 0)

    def run(k, _):
        lo = (k - 1) * c
        w_slot = lax.rem(k, 2)
        at_point(k, None)
        for k0 in range(2, len(runs)):

            @pl.when(k == k0)
            def _(k0=k0):
                wait(load(k0))

        def tile(i, _):
            at_point(k, i)
            slot = lax.rem(i, 2)

            @pl.when(i >= 2)
            def _():
                wait(o_copies(slot, i - 2, lo, c))

            @pl.when(jnp.logical_and(i < 2, k == 2))
            def _():
                wait(o_copies(slot, i + 2, *runs[1]))

            @pl.when(jnp.logical_and(i < 2, k > 2))
            def _():
                wait(o_copies(slot, i + 2, lo - c, c))

            compute(i, lo, c, pieces(c), w_slot)
            return 0

        lax.fori_loop(0, 4, tile, 0)
        return 0

    lax.fori_loop(2, len(runs), run, 0)
    last = len(runs) - 1
    wait(load_d())
    before = {
        0: lambda: h3(g1),
        3: lambda: h2(u1),
        4: lambda: h3(u1),
        5: lambda: h1(d1),
    }

    def norm_of(m):
        wide = ho_v[lax.rem(m, 2)].astype(F32)
        ao_v[lax.rem(m, 2)] = (wide * scale_of(wide)).astype(BF)

    def tile(m, _):
        slot = lax.rem(m, 2)

        @pl.when(m == 3)
        def _():
            wait(o_copies(0, 2, *runs[last]))
            wait(o_copies(1, 3, *runs[last]))

        @pl.when(m < 7)
        def _():
            start(i_copies(m + 1))

        for m0, do in before.items():
            guarded(m == m0, do)
        wait(i_copies(m))

        @pl.when(m > 1)
        def _():
            wait(h_copy(m - 2))

        @pl.when(m > 2)
        def _():
            wait(a1_copy(m - 3))

        norm_of(m + 1)
        ho_v[slot] = (xi_v[slot].astype(F32) + dot(hi_v[slot], wd_v[...]).astype(BF).astype(F32)).astype(BF)
        start(h_copy(m))

        @pl.when(m > 0)
        def _():
            start(a1_copy(m - 1))

        return 0

    lax.fori_loop(0, 8, tile, 0)
    wait(a1_copy(5))
    norm_of(7)
    start(a1_copy(7))
    wait(h_copy(6))
    wait(h_copy(7))
    wait(a1_copy(6))
    wait(a1_copy(7))
    for i in range(8):
        wait(a_copy(i))
    h2(d1)
    h3(d1)


def forward(x, wg, wu, wd):
    t, d = x.shape
    f = wg.shape[2]
    c = f // CHUNKS
    n, dma = 2 * CHUNKS + 6, pltpu.SemaphoreType.DMA
    shapes = [((t, d), BF), ((t, f), BF), ((t, f), F32), ((t, f), F32), ((t, d), BF), ((t, d), BF)]
    shapes += [((2, d, f), BF), ((2, d, f), BF), ((2, f, d), BF)]
    return pl.pallas_call(
        forward_kernel,
        in_specs=[ANY] * 4,
        out_specs=[ANY] * len(shapes),
        out_shape=[jax.ShapeDtypeStruct(*s) for s in shapes],
        scratch_shapes=[
            pltpu.VMEM((t, d), BF),
            pltpu.VMEM((2, d, 2 * c), BF),
            pltpu.VMEM((4, t // 8, d), BF),
            pltpu.VMEM((2, t // 4, c), BF),
            pltpu.VMEM((2, t // 4, c), F32),
            pltpu.VMEM((2, t // 4, c), F32),
            pltpu.VMEM((f, d), BF),
            pltpu.VMEM((2, t // 8, f), BF),
            pltpu.VMEM((2, t // 8, d), BF),
            pltpu.VMEM((2, t // 8, d), BF),
            pltpu.VMEM((2, t // 8, d), BF),
            pltpu.VMEM(wg.shape[1:], BF),
            pltpu.VMEM(wd.shape[1:], BF),
            dma((2, n, 2)),
            dma((2, n, 3)),
            dma((2, n, 2)),
            dma((2, 2)),
            dma((2, 2)),
            dma((4,)),
            dma((8,)),
            dma((2, 3)),
            dma,
            dma((2, 2)),
            dma((2, 2)),
        ],
        compiler_params=pltpu.CompilerParams(vmem_limit_bytes=VMEM_LIMIT, collective_id=2, has_side_effects=True),
        cost_estimate=pl.CostEstimate(flops=6 * t * d * f, bytes_accessed=16 * t * f, transcendentals=t * f),
        name="forward",
    )(x, wg, wu, wd)


def backward_kernel(layer, *refs):
    saved = layer == 0
    n_in = 9 if saved else 6
    a_hbm, h_hbm, dy_hbm, wg_hbm, wu_hbm, wd_hbm = refs[:6]
    g_hbm, u_hbm, hid_hbm = refs[6:n_in] if saved else (None, None, None)
    out_hbm, og_hbm, ou_hbm, od_hbm, dgu_hbm, dwd_hbm = refs[n_in : n_in + 6]
    (stg, buf_d, acc, buf_x, s_x, s_r, buf_r, s_g, sem_d, sem_x, sem_r, sem_g, sem_gl, free_d, free_x, free_r, entered) = refs[n_in + 6 :]

    t, d = a_hbm.shape
    f = wd_hbm.shape[1]
    c = f // CHUNKS
    own = d // 4
    quarter = own // 4
    own_d = f // 4
    rd = own_d // 5
    qd = d // 4
    me_r, x, core = here()
    partner, across, peers = neighbours()
    everyone = [partner, across] + [p for _, p in peers]
    meet(everyone)

    def d_copies():
        return [
            send(stg.at[rows((2 * k + 1 - core) * own, own), :], buf_d.at[k], (sem_d.at[0, k], sem_d.at[1, k]), partner)
            for k in range(2)
        ]

    def x_copies():
        return [send(s_x, buf_x, (sem_x.at[0], sem_x.at[1]), across)]

    def r_copies():
        return [
            send(s_r.at[rows(n * quarter, quarter), :], buf_r.at[k], (sem_r.at[0, k], sem_r.at[1, k]), p)
            for k, (n, p) in enumerate(peers)
        ]

    def g_copies(p):
        at = (rows(me_r * quarter, quarter), rows(p * c, c, 128))
        far = [
            send(s_g.at[:, pl.ds(i * c, c)], o.at[at], (sem_g.at[0, lax.rem(p, 2), i, k], sem_g.at[1, lax.rem(p, 2), i, k]), to)
            for k, (_, to) in enumerate(peers)
            for i, o in enumerate((og_hbm, ou_hbm))
        ]
        near = [pltpu.make_async_copy(s_g.at[:, pl.ds(i * c, c)], o.at[at], sem_gl.at[i]) for i, o in enumerate((og_hbm, ou_hbm))]
        return far + near

    def e0(p, first):
        if not first:
            pl.semaphore_wait(free_d, 1)
        start(d_copies())

    def e1(p, first, last):
        wait(d_copies())
        acc[lax.rem(p, 2)] = stg[rows((2 * x + core) * own, own), :].astype(F32) + buf_d[x].astype(F32)
        s_x[...] = (stg[rows((2 * (1 - x) + core) * own, own), :].astype(F32) + buf_d[1 - x].astype(F32)).astype(BF)
        if not last:
            pl.semaphore_signal(free_d, inc=1, device_id=partner, device_id_type=MESH)
        if not first:
            pl.semaphore_wait(free_x, 1)
        start(x_copies())

    def e2(p, first, last):
        wait(x_copies())
        total = acc[lax.rem(p, 2)] + buf_x[...].astype(F32)
        acc[lax.rem(p, 2)] = total
        s_r[...] = total.astype(BF)
        if not last:
            pl.semaphore_signal(free_x, inc=1, device_id=across, device_id_type=MESH)
        if not first:
            for k in range(3):
                pl.semaphore_wait(free_r.at[k], 1)
        start(r_copies())

    def e3(p, last):
        wait(r_copies())
        total = acc[lax.rem(p, 2), rows(me_r * quarter, quarter), :]
        for k in range(3):
            total = total + buf_r[k].astype(F32)
        s_g[...] = total.astype(BF)
        if not last:
            for k, (_, to) in enumerate(peers):
                pl.semaphore_signal(free_r.at[2 - k], inc=1, device_id=to, device_id_type=MESH)
        start(g_copies(p))

    def e4(p):
        wait(g_copies(p))

    tm = t // 4
    tiles = t // tm

    def chunks(*bufs):
        if saved:
            a_v, dy_v, wd_v, hid_v, dgs, dst, g_v, u_v, sem_a, sem_w, sem_o, sem_s, sem_h = bufs
        else:
            a_v, dy_v, wd_v, hid_v, dgs, dst, wgu_v, sem_a, sem_w, sem_o = bufs

        def a_copies(i):
            at = rows(i * tm, tm)
            return [
                pltpu.make_async_copy(a_hbm.at[at, :], a_v.at[at, :], sem_a.at[0, i]),
                pltpu.make_async_copy(dy_hbm.at[at, :], dy_v.at[at, :], sem_a.at[1, i]),
            ]

        def w_copies(j):
            slot = lax.rem(j, 2)
            at = rows(j * c, c, 128)
            w = [pltpu.make_async_copy(wd_hbm.at[layer, at, :], wd_v.at[slot], sem_w.at[slot, 0])]
            if not saved:
                w.append(pltpu.make_async_copy(wg_hbm.at[layer, :, at], wgu_v.at[slot, :, pl.ds(0, c)], sem_w.at[slot, 1]))
                w.append(pltpu.make_async_copy(wu_hbm.at[layer, :, at], wgu_v.at[slot, :, pl.ds(c, c)], sem_w.at[slot, 2]))
            return w

        def s_copies(n):
            slot = lax.rem(n, 2)
            at = (rows(lax.rem(n, tiles) * tm, tm), rows(lax.div(n, tiles) * c, c, 128))
            return [
                pltpu.make_async_copy(g_hbm.at[at], g_v.at[slot], sem_s.at[slot, 0]),
                pltpu.make_async_copy(u_hbm.at[at], u_v.at[slot], sem_s.at[slot, 1]),
            ]

        def o_copies(j):
            return [
                pltpu.make_async_copy(dgs.at[:, pl.ds(0, c)], dgu_hbm.at[:, rows(j * c, c, 128)], sem_o.at[0]),
                pltpu.make_async_copy(dgs.at[:, pl.ds(c, c)], dgu_hbm.at[:, rows(f + j * c, c, 128)], sem_o.at[1]),
            ]

        def hid_copy(j):
            return [pltpu.make_async_copy(hid_hbm.at[:, rows(j * c, c, 128)], hid_v, sem_h)]

        def dw_copy(j):
            return [pltpu.make_async_copy(dst, dwd_hbm.at[rows(j * c, c), :], sem_o.at[2])]

        start(w_copies(0))
        for i in range(tiles):
            start(a_copies(i))
            if saved and i == 0:
                start(s_copies(0))
        if saved:
            start(hid_copy(0))

        def chunk(j, _):
            slot = lax.rem(j, 2)

            @pl.when(j >= 3)
            def _():
                e4(j - 3)

            @pl.when(j == 2)
            def _():
                e2(j - 2, True, False)

            @pl.when(j >= 3)
            def _():
                e2(j - 2, False, False)

            @pl.when(j == 1)
            def _():
                e0(j - 1, True)

            @pl.when(j >= 2)
            def _():
                e0(j - 1, False)

            @pl.when(j >= 1)
            def _():
                wait(o_copies(j - 1))

            wait(w_copies(j))

            @pl.when(j + 1 < CHUNKS)
            def _():
                start(w_copies(j + 1))

            def tile(i, _):
                @pl.when(j == 0)
                def _():
                    wait(a_copies(i))

                if saved:
                    n = j * tiles + i

                    @pl.when(n + 1 < CHUNKS * tiles)
                    def _():
                        start(s_copies(n + 1))

                    wait(s_copies(n))

                @pl.when(jnp.logical_and(i == tiles // 2, j == 1))
                def _():
                    e1(j - 1, True, False)

                @pl.when(jnp.logical_and(i == tiles // 2, j >= 2))
                def _():
                    e1(j - 1, False, False)

                r = rows(i * tm, tm)
                for p0, w in pieces(c):
                    if not saved:
                        a = a_v[r, :]
                        both = dot(a, jnp.concatenate([wgu_v[slot, :, pl.ds(p0, w)], wgu_v[slot, :, pl.ds(c + p0, w)]], 1))
                        g, u = both[:, :w], both[:, w:]
                    dh = dot(dy_v[r, :], wd_v[slot, pl.ds(p0, w), :], NT).astype(BF).astype(F32)
                    if saved:
                        by_gate, by_up = g_v[lax.rem(n, 2), :, pl.ds(p0, w)], u_v[lax.rem(n, 2), :, pl.ds(p0, w)]
                    else:
                        s = jax.nn.sigmoid(g)
                        by_up = g * s
                        by_gate = u * (s + by_up * (1.0 - s))
                        hid_v[r, pl.ds(p0, w)] = (by_up * u).astype(BF)
                    dgs[r, pl.ds(c + p0, w)] = (dh * by_up).astype(BF)
                    dgs[r, pl.ds(p0, w)] = (dh * by_gate).astype(BF)
                return 0

            lax.fori_loop(0, tiles, tile, 0)
            start(o_copies(j))

            @pl.when(j >= 1)
            def _():
                wait(dw_copy(j - 1))

            if saved:
                wait(hid_copy(j))
            for p0, w in pieces(c):
                dst[pl.ds(p0, w), :] = dot(hid_v[:, pl.ds(p0, w)], dy_v[...], TN).astype(BF)
            start(dw_copy(j))
            if saved:

                @pl.when(j + 1 < CHUNKS)
                def _():
                    start(hid_copy(j + 1))

            @pl.when(j >= 2)
            def _():
                e3(j - 2, False)

            for k in range(2):
                stg[pl.ds(k * (d // 2), d // 2), :] = dot(a_v[:, pl.ds(k * (d // 2), d // 2)], dgs[...], TN).astype(BF)
            return 0

        lax.fori_loop(0, CHUNKS, chunk, 0)
        wait(o_copies(CHUNKS - 1))
        wait(dw_copy(CHUNKS - 1))

    bufs = [
        pltpu.VMEM((t, d), BF),
        pltpu.VMEM((t, d), BF),
        pltpu.VMEM((2, c, d), BF),
        pltpu.VMEM((t, c), BF),
        pltpu.VMEM((t, 2 * c), BF),
        pltpu.VMEM((c, d), BF),
    ]
    bufs += [pltpu.VMEM((2, tm, c), F32)] * 2 if saved else [pltpu.VMEM((2, d, 2 * c), BF)]
    bufs += [pltpu.SemaphoreType.DMA((2, tiles)), pltpu.SemaphoreType.DMA((2, 3)), pltpu.SemaphoreType.DMA((3,))]
    bufs += [pltpu.SemaphoreType.DMA((2, 2)), pltpu.SemaphoreType.DMA] if saved else []
    pl.run_scoped(chunks, *bufs)

    ta = t // 8

    def last(wg_v, wu_v, dgu_v, h_v, dy_v, o_v, bg_v, bu_v, own_v, bd_v, ac_v, bx_v, sx_v, br_v, sg_v, sem_w, sem_i, sem_o, dd, dx, dr, dg, dl):
        def i_copy(i, m):
            slot = lax.rem(i, 2)
            part = pl.ds(m * f, f)
            return pltpu.make_async_copy(dgu_hbm.at[rows(i * ta, ta), part], dgu_v.at[slot, :, part], sem_i.at[slot, m])

        def i_copies(i):
            return [i_copy(i, 0), i_copy(i, 1)]

        def h_copies(i):
            slot = lax.rem(i, 2)
            at = rows(i * ta, ta)
            return [
                pltpu.make_async_copy(h_hbm.at[at, :], h_v.at[slot], sem_i.at[slot, 2]),
                pltpu.make_async_copy(dy_hbm.at[at, :], dy_v.at[slot], sem_i.at[slot, 3]),
            ]

        def o_copy(i):
            slot = lax.rem(i, 2)
            return [pltpu.make_async_copy(o_v.at[slot], out_hbm.at[rows(i * ta, ta), :], sem_o.at[slot])]

        def w_copy(k):
            return [pltpu.make_async_copy((wg_hbm, wu_hbm)[k].at[layer], (wg_v, wu_v)[k], sem_w.at[k])]

        def dd_copies(k):
            far = [
                send(
                    dwd_hbm.at[rows((2 * m + 1 - core) * own_d + k * rd, rd), :],
                    bd_v.at[k, m],
                    (dd.at[0, k, m], dd.at[1, k, m]),
                    partner,
                )
                for m in range(2)
            ]
            near = [
                pltpu.make_async_copy(dwd_hbm.at[rows((2 * m + core) * own_d + k * rd, rd), :], own_v.at[k, m], dl.at[0, k, m])
                for m in range(2)
            ]
            return far + near

        def dx_copies(k):
            return [send(sx_v.at[k], bx_v.at[k], (dx.at[0, k], dx.at[1, k]), across)]

        def dr_copies(k):
            return [
                send(sx_v.at[k, :, rows(n * qd, qd, 128)], br_v.at[k, m], (dr.at[0, k, m], dr.at[1, k, m]), to)
                for m, (n, to) in enumerate(peers)
            ]

        def dg_copies(k):
            at = (rows(k * rd, rd), rows(me_r * qd, qd, 128))
            far = [send(sg_v.at[k], od_hbm.at[at], (dg.at[0, k, m], dg.at[1, k, m]), to) for m, (_, to) in enumerate(peers)]
            return far + [pltpu.make_async_copy(sg_v.at[k], od_hbm.at[at], dl.at[1, k, 0])]

        def f0(k):
            start(dd_copies(k))

        def f1(k):
            wait(dd_copies(k))
            ac_v[k] = own_v[k, x].astype(F32) + bd_v[k, x].astype(F32)
            sx_v[k] = (own_v[k, 1 - x].astype(F32) + bd_v[k, 1 - x].astype(F32)).astype(BF)
            start(dx_copies(k))

        def f2(k):
            wait(dx_copies(k))
            total = ac_v[k] + bx_v[k].astype(F32)
            ac_v[k] = total
            sx_v[k] = total.astype(BF)
            start(dr_copies(k))

        def f3(k):
            wait(dr_copies(k))
            total = ac_v[k, :, rows(me_r * qd, qd, 128)]
            for m in range(3):
                total = total + br_v[k, m].astype(F32)
            sg_v[k] = total.astype(BF)
            start(dg_copies(k))

        def f4(k):
            wait(dg_copies(k))

        end = CHUNKS - 1
        todo = {
            1: [lambda: f1(0), lambda: f1(1)],
            2: [lambda: e3(end - 1, False), lambda: f1(2)],
            3: [lambda: f1(3), lambda: f1(4)],
            5: [lambda: e2(end, False, True), lambda: e4(end - 1)],
            7: [lambda: f2(0)],
            8: [lambda: e3(end, True), lambda: f2(1)],
            10: [lambda: f2(2), lambda: f3(0)],
            11: [lambda: e4(end), lambda: f3(1)],
            12: [lambda: f2(3)],
            13: [lambda: f3(2)],
            14: [lambda: f2(4)],
            15: [lambda: f3(3)],
        }

        def events(i, half):
            for point, does in todo.items():
                if point % 2 == half:

                    @pl.when(i == point // 2)
                    def _(does=does):
                        for do in does:
                            do()

        def tail(i):
            slot = lax.rem(i, 2)
            by_a = (bg_v[...].astype(F32) + bu_v[...].astype(F32)).astype(BF).astype(F32)
            wide = h_v[slot].astype(F32)
            scale = scale_of(wide)
            by_scale = jnp.sum(by_a * wide, -1, keepdims=True)
            by_wide = (by_a * scale - (by_scale * scale * scale * scale * (1.0 / d)) * wide).astype(BF)
            o_v[slot] = (dy_v[slot].astype(F32) + by_wide.astype(F32)).astype(BF)

        def by_g(i):
            bg_v[...] = dot(dgu_v[lax.rem(i, 2), :, pl.ds(0, f)], wg_v[...], NT).astype(BF)

        def by_u(i):
            bu_v[...] = dot(dgu_v[lax.rem(i, 2), :, pl.ds(f, f)], wu_v[...], NT).astype(BF)

        start(w_copy(0))
        i_copy(0, 0).start()
        start(w_copy(1))
        i_copy(0, 1).start()
        start(h_copies(0))
        for p in everyone:
            pl.semaphore_signal(entered, inc=1, device_id=p, device_id_type=MESH)
        e4(end - 2)
        e2(end - 1, False, False)
        e0(end, False)
        wait(w_copy(0))
        i_copy(0, 0).wait()
        pl.semaphore_wait(entered, 5)
        for k in range(5):
            f0(k)
        e1(end, False, True)
        start(i_copies(1))
        by_g(0)
        events(0, 1)
        wait(w_copy(1))
        i_copy(0, 1).wait()
        by_u(0)

        def tile(i, _):
            @pl.when(i + 1 < 8)
            def _():
                start(i_copies(i + 1))

            events(i, 0)
            wait(i_copies(i))
            wait(h_copies(i - 1))

            @pl.when(i >= 3)
            def _():
                wait(o_copy(i - 3))

            tail(i - 1)
            by_g(i)
            start(o_copy(i - 1))
            start(h_copies(i))
            events(i, 1)
            by_u(i)
            return 0

        lax.fori_loop(1, 8, tile, 0)
        f3(4)
        wait(h_copies(7))
        wait(o_copy(5))
        tail(7)
        start(o_copy(7))
        wait(o_copy(6))
        wait(o_copy(7))
        for k in range(5):
            f4(k)

    pl.run_scoped(
        last,
        pltpu.VMEM((d, f), BF),
        pltpu.VMEM((d, f), BF),
        pltpu.VMEM((2, ta, 2 * f), BF),
        pltpu.VMEM((2, ta, d), BF),
        pltpu.VMEM((2, ta, d), BF),
        pltpu.VMEM((2, ta, d), BF),
        pltpu.VMEM((ta, d), BF),
        pltpu.VMEM((ta, d), BF),
        pltpu.VMEM((5, 2, rd, d), BF),
        pltpu.VMEM((5, 2, rd, d), BF),
        pltpu.VMEM((5, rd, d), F32),
        pltpu.VMEM((5, rd, d), BF),
        pltpu.VMEM((5, rd, d), BF),
        pltpu.VMEM((5, 3, rd, qd), BF),
        pltpu.VMEM((5, rd, qd), BF),
        pltpu.SemaphoreType.DMA((2,)),
        pltpu.SemaphoreType.DMA((2, 4)),
        pltpu.SemaphoreType.DMA((2,)),
        pltpu.SemaphoreType.DMA((2, 5, 2)),
        pltpu.SemaphoreType.DMA((2, 5)),
        pltpu.SemaphoreType.DMA((2, 5, 3)),
        pltpu.SemaphoreType.DMA((2, 5, 3)),
        pltpu.SemaphoreType.DMA((2, 5, 2)),
    )


def backward(a, h, dy, wg, wu, wd, saved, layer):
    t, d = a.shape
    f = wd.shape[1]
    c = f // CHUNKS
    own, dma = d // 4, pltpu.SemaphoreType.DMA
    shapes = [(t, d), (own, f), (own, f), (f // 4, d), (t, 2 * f), (f, d)]
    out = pl.pallas_call(
        functools.partial(backward_kernel, layer),
        in_specs=[ANY] * (9 if saved is not None else 6),
        out_specs=[ANY] * len(shapes),
        out_shape=[jax.ShapeDtypeStruct(s, BF) for s in shapes],
        scratch_shapes=[
            pltpu.VMEM((d, 2 * c), BF),
            pltpu.VMEM((2, own, 2 * c), BF),
            pltpu.VMEM((2, own, 2 * c), F32),
            pltpu.VMEM((own, 2 * c), BF),
            pltpu.VMEM((own, 2 * c), BF),
            pltpu.VMEM((own, 2 * c), BF),
            pltpu.VMEM((3, own // 4, 2 * c), BF),
            pltpu.VMEM((own // 4, 2 * c), BF),
            dma((2, 2)),
            dma((2,)),
            dma((2, 3)),
            dma((2, 2, 2, 3)),
            dma((2,)),
            pltpu.SemaphoreType.REGULAR,
            pltpu.SemaphoreType.REGULAR,
            pltpu.SemaphoreType.REGULAR((3,)),
            pltpu.SemaphoreType.REGULAR,
        ],
        compiler_params=pltpu.CompilerParams(vmem_limit_bytes=VMEM_LIMIT, collective_id=layer, has_side_effects=True),
        cost_estimate=pl.CostEstimate(
            flops=(12 if saved is not None else 16) * t * d * f, bytes_accessed=30 * t * f, transcendentals=t * f
        ),
        name=f"backward_{layer}",
    )(a, h, dy, wg, wu, wd, *(saved or ()))
    return out[:4]


def placed_kernel(*refs):
    ins, outs = refs[:7], refs[7:11]
    bufs, sem_in, sem_out = refs[11:18], refs[18], refs[19]
    parts = 8
    copies = []
    for n, (src, buf) in enumerate(zip(ins, bufs, strict=True)):
        dst = outs[0] if n == 0 else outs[(n + 1) // 2].at[(n - 1) % 2]
        step = src.shape[0] // (parts if n == 0 else 1)
        for p in range(parts if n == 0 else 1):
            at = pl.ds(p * step, step)
            k = len(copies)
            copies.append(
                (
                    pltpu.make_async_copy(src.at[at, :], buf.at[at, :], sem_in.at[k]),
                    pltpu.make_async_copy(buf.at[at, :], dst.at[at, :], sem_out.at[k]),
                )
            )
    for first, _ in copies:
        first.start()
    for first, second in copies:
        first.wait()
        second.start()
    for _, second in copies:
        second.wait()


def placed(by_x, *sums):
    ins = (by_x, *sums)
    outs = [by_x.shape] + [(2, *s.shape) for s in sums[::2]]
    return pl.pallas_call(
        placed_kernel,
        in_specs=[ANY] * len(ins),
        out_specs=[ANY] * len(outs),
        out_shape=[jax.ShapeDtypeStruct(s, BF) for s in outs],
        scratch_shapes=[pltpu.VMEM(a.shape, BF) for a in ins]
        + [pltpu.SemaphoreType.DMA((14,)), pltpu.SemaphoreType.DMA((14,))],
        compiler_params=pltpu.CompilerParams(vmem_limit_bytes=VMEM_LIMIT),
        name="placed",
    )(*ins)


def solution(mesh):
    def step(x, dy, *weights):
        x, dy = x[0], dy[0]
        a0, hid, g, u, h, a1, *whole = forward(x, *weights)
        by_h, *top = backward(a1, h, dy, *whole, None, 1)
        by_x, *bottom = backward(a0, x, by_h, *whole, (g, u, hid), 0)
        by_x, *sums = placed(by_x, *(part for pair in zip(bottom, top, strict=True) for part in pair))
        return (by_x[None], *sums)

    states, cut = P(("rep", "r", "s"), None, None), P(None, "s", None)
    return jax.shard_map(
        step,
        mesh=mesh,
        in_specs=(states, states) + (cut,) * 3,
        out_specs=(states,) + (P("rep", "s", None),) * 3,
        check_vma=False,
    )
```

```python
import functools

import jax
import jax.numpy as jnp
from jax import lax
from jax.experimental import pallas as pl
from jax.experimental.pallas import tpu as pltpu
from jax.sharding import PartitionSpec as P

BF, F32 = jnp.bfloat16, jnp.float32
MESH = pl.DeviceIdType.MESH
NT = (((1,), (1,)), ((), ()))
TN = (((0,), (0,)), ((), ()))
ANY = pl.BlockSpec(memory_space=pl.ANY)
CHUNKS = 5
VMEM_LIMIT = 67043328


def dot(a, b, dims=(((1,), (0,)), ((), ()))):
    return lax.dot_general(a, b, dims, preferred_element_type=F32)


def scale_of(wide):
    return lax.rsqrt(jnp.mean(wide * wide, -1, keepdims=True) + 1e-6)


def pieces(width):
    first = 256 if width > 512 else width // 2
    return ((0, first), (first, width - first))


def rows(start, size, unit=16):
    return pl.ds(pl.multiple_of(start, unit) if size % unit == 0 else start, size)


def here():
    s = lax.axis_index("s")
    return lax.axis_index("r"), lax.div(s, 2), lax.rem(s, 2)


def send(src, dst, sems, to):
    return pltpu.make_async_remote_copy(
        src_ref=src, dst_ref=dst, send_sem=sems[0], recv_sem=sems[1], device_id=to, device_id_type=MESH
    )


def start(copies):
    for copy in copies:
        copy.start()


def wait(copies):
    for copy in copies:
        copy.wait()


def guarded(condition, do):
    @pl.when(condition)
    def _():
        do()


def neighbours():
    me_r, x, core = here()
    partner = {"s": x * 2 + (1 - core)}
    across = {"s": (1 - x) * 2 + core}
    peers = [(lax.rem(me_r + k, 4), {"r": lax.rem(me_r + k, 4)}) for k in (1, 2, 3)]
    return partner, across, peers


def meet(everyone):
    barrier = pltpu.get_barrier_semaphore()
    for p in everyone:
        pl.semaphore_signal(barrier, inc=1, device_id=p, device_id_type=MESH)
    pl.semaphore_wait(barrier, len(everyone))


def forward_kernel(x_hbm, wg_own, wu_own, wd_own, *refs):
    a_hbm, hid_hbm, g_hbm, u_hbm, h_hbm, a1_hbm, wg_all, wu_all, wd_all = refs[:9]
    (a_v, w_v, x_v, hid_v, g_v, u_v, wd_v, hi_v, xi_v, ho_v, ao_v, bg_v, bd_v) = refs[9:22]
    sem_x, sem_y, sem_d, sem_b, sem_w, sem_i, sem_ao, sem_o, sem_wd, sem_p, sem_q = refs[22:]
    t, d = x_hbm.shape
    f = hid_hbm.shape[1]
    c = f // CHUNKS
    me_r, x, core = here()
    me, oa = 2 * x + core, 2 * (1 - x) + core
    partner, across, peers = neighbours()
    p0 = 256 if c > 512 else c // 2
    runs = [(0, p0), (p0, c - p0)] + [(c * k, c) for k in range(1, CHUNKS)]

    class Piece:
        def __init__(self, number, layer, own, full, lo, width):
            self.n = number
            held = own.shape[1]
            unit = 16 if held >= 128 else 4
            self.q = held * 3 // 16 // unit * unit
            self.direct = held - 4 * self.q
            self.held = held
            self.own = lambda at, size: own.at[layer, rows(at, size), pl.ds(lo, width)]
            self.full = lambda at, size: full.at[layer, rows(at, size), pl.ds(lo, width)]

        def quarter(self):
            at, to = self.direct + me_r * self.q, me * self.held
            return send(self.own(at, self.q), self.full(to + at, self.q), (sem_x.at[0, self.n, 0], sem_x.at[1, self.n, 0]), across)

        def straight(self):
            sems = (sem_x.at[0, self.n, 1], sem_x.at[1, self.n, 1])
            return send(self.own(0, self.direct), self.full(me * self.held, self.direct), sems, across)

        def y_copies(self):
            block = self.full(oa * self.held + self.direct + me_r * self.q, self.q)
            return [send(block, block, (sem_y.at[0, self.n, k], sem_y.at[1, self.n, k]), to) for k, (_, to) in enumerate(peers)]

        def mine(self):
            sems = (sem_d.at[0, self.n, 0], sem_d.at[1, self.n, 0])
            return send(self.own(0, self.held), self.full(me * self.held, self.held), sems, partner)

        def theirs(self):
            block = self.full(oa * self.held, self.held)
            return send(block, block, (sem_d.at[0, self.n, 1], sem_d.at[1, self.n, 1]), partner)

    gate_up = [
        [Piece(2 * p + m, 0, own, full, lo, width) for m, (own, full) in enumerate(((wg_own, wg_all), (wu_own, wu_all)))]
        for p, (lo, width) in enumerate(runs)
    ]
    n = 2 * len(runs)
    d0, g1, u1, d1 = (
        [Piece(n, 0, wd_own, wd_all, 0, d)],
        [Piece(n + 1, 1, wg_own, wg_all, 0, f)],
        [Piece(n + 2, 1, wu_own, wu_all, 0, f)],
        [Piece(n + 3, 1, wd_own, wd_all, 0, d)],
    )

    def h0(group):
        for p in group:
            p.quarter().start()
            p.straight().start()
        for p in group:
            p.mine().start()

    def h1(group):
        for p in group:
            p.quarter().wait()
            start(p.y_copies())

    def h2(group):
        for p in group:
            p.straight().wait()
            wait(p.y_copies())
            p.theirs().start()

    def h3(group):
        for p in group:
            p.mine().wait()
            p.theirs().wait()

    blocks = [(wg_own, wg_all, bg_v), (wu_own, wu_all, bg_v), (wd_own, wd_all, bd_v)]

    def b_in(layer, m):
        own, _, via = blocks[m]
        return pltpu.make_async_copy(own.at[layer], via, sem_b.at[m // 2, 0])

    def b_out(layer, m):
        own, full, via = blocks[m]
        return pltpu.make_async_copy(via, full.at[layer, rows(me * own.shape[1], own.shape[1]), :], sem_b.at[m // 2, 1])

    def b0(layer, m):
        b_in(layer, m).start()

    def b1(layer, m):
        b_in(layer, m).wait()
        b_out(layer, m).start()

    def b2(layer, m):
        b_out(layer, m).wait()

    def load(k):
        lo, width = runs[k]
        at = pl.ds(lo, width)
        return [
            pltpu.make_async_copy(full.at[0, :, at], w_v.at[k % 2, :, pl.ds(m * c, width)], sem_w.at[k % 2, m])
            for m, full in enumerate((wg_all, wu_all))
        ]

    def load_d():
        return [pltpu.make_async_copy(wd_all.at[0], wd_v, sem_wd)]

    tm = t // 4
    td = t // 8
    tn = min(64, td)

    def x_copy(i):
        return [pltpu.make_async_copy(x_hbm.at[rows(i * td, td), :], x_v.at[i % 4], sem_i.at[i % 4])]

    def a_copy(i):
        return [pltpu.make_async_copy(a_v.at[rows(i * td, td), :], a_hbm.at[rows(i * td, td), :], sem_ao.at[i])]

    for i in range(4):
        start(x_copy(i))
    b0(0, 0)
    b0(0, 2)
    meet([partner, across] + [p for _, p in peers])
    h0(gate_up[0])
    h0(gate_up[1])
    h0(gate_up[2])
    for i in range(8):
        wait(x_copy(i))

        def norm(k, _, i=i):
            wide = x_v[i % 4, rows(k * tn, tn), :].astype(F32)
            a_v[rows(i * td + k * tn, tn), :] = (wide * scale_of(wide)).astype(BF)
            return 0

        lax.fori_loop(0, td // tn, norm, 0)
        start(a_copy(i))
        if i < 4:
            start(x_copy(i + 4))
        if i == 1:
            b1(0, 0)
            b1(0, 2)
        if i == 2:
            h1(gate_up[0])
            b2(0, 0)
            b0(0, 1)
        if i == 4:
            b1(0, 1)
            h1(gate_up[1])
        if i == 5:
            h2(gate_up[0])
            b2(0, 1)
            h0(gate_up[3])
    h3(gate_up[0])
    start(load(0))
    h0(gate_up[4])

    def o_copies(slot, i, lo, width):
        at = (rows(i * tm, tm), rows(lo, width, 128))
        near = pl.ds(0, width)
        return [
            pltpu.make_async_copy(v.at[slot, :, near], o.at[at], sem_o.at[slot, m])
            for m, (v, o) in enumerate(((hid_v, hid_hbm), (g_v, g_hbm), (u_v, u_hbm)))
        ]

    def compute(i, lo, width, parts, w_slot):
        slot = lax.rem(i, 2)
        a = a_v[rows(i * tm, tm), :]
        for at, w in parts:
            both = dot(a, jnp.concatenate([w_v[w_slot, :, pl.ds(at, w)], w_v[w_slot, :, pl.ds(c + at, w)]], 1))
            g, u = both[:, :w], both[:, w:]
            s = jax.nn.sigmoid(g)
            silu = g * s
            g_v[slot, :, pl.ds(at, w)] = u * (s + silu * (1.0 - s))
            u_v[slot, :, pl.ds(at, w)] = silu
            hid_v[slot, :, pl.ds(at, w)] = (silu * u).astype(BF)
        start(o_copies(slot, i, lo, width))

    def i_copies(m):
        at = rows(m * td, td)
        return [
            pltpu.make_async_copy(hid_hbm.at[at, :], hi_v.at[lax.rem(m, 2)], sem_p.at[lax.rem(m, 2), 0]),
            pltpu.make_async_copy(x_hbm.at[at, :], xi_v.at[lax.rem(m, 2)], sem_p.at[lax.rem(m, 2), 1]),
        ]

    def h_copy(m):
        return [pltpu.make_async_copy(ho_v.at[lax.rem(m, 2)], h_hbm.at[rows(m * td, td), :], sem_q.at[lax.rem(m, 2), 0])]

    def a1_copy(m):
        return [pltpu.make_async_copy(ao_v.at[lax.rem(m, 2)], a1_hbm.at[rows(m * td, td), :], sem_q.at[lax.rem(m, 2), 1])]

    gu = gate_up
    before = {
        (0, 1): lambda: (b0(1, 0), b2(0, 2), b0(1, 2)),
        (0, 2): lambda: (h2(gu[1]), h1(gu[2])),
        (0, 3): lambda: (h3(gu[1]), start(load(1)), h0(gu[5])),
        (1, 0): lambda: (b1(1, 0), b1(1, 2)),
        (1, 1): lambda: (h2(gu[2]), h1(gu[3]), h0(d0)),
        (1, 2): lambda: (h3(gu[2]), start(load(2))),
        (1, 3): lambda: (b2(1, 0), b0(1, 1), b2(1, 2)),
        (2, 0): lambda: (h2(gu[3]), h1(gu[4]), b1(1, 1), h0(g1)),
        (2, 1): lambda: (h3(gu[3]), start(load(3))),
        (2, 2): lambda: h1(gu[5]),
        (2, 3): lambda: (h2(gu[4]), b2(1, 1)),
        (3, 0): lambda: (h3(gu[4]), start(load(4)), h0(u1)),
        (3, 1): lambda: (h2(gu[5]), h1(d0)),
        (3, 2): lambda: h3(gu[5]),
        (4, 0): lambda: (start(load(5)), h0(d1)),
        (4, 2): lambda: (h2(d0), h1(g1)),
        (5, 0): lambda: (h3(d0), start(load_d())),
        (5, 2): lambda: (h2(g1), h1(u1)),
        (5, 3): lambda: start(i_copies(0)),
    }

    def at_point(k, i):
        for (k0, i0), do in before.items():
            if isinstance(k, int):
                if k0 == k and i0 >= 0:
                    guarded(i == i0, do)
            elif k0 > 1 and (i0 < 0) == (i is None):
                guarded(k == k0 if i is None else jnp.logical_and(k == k0, i == i0), do)

    for k in (0, 1):
        lo, width = runs[k]
        first = max(width // 2 // 128 * 128, width // 2 if width < 256 else 0)
        wait(load(k))

        def tile(i, _, k=k, lo=lo, width=width, first=first):
            at_point(k, i)
            slot = lax.rem(i, 2)

            @pl.when(i >= 2)
            def _():
                wait(o_copies(slot, i - 2, lo, width))

            if k == 1:

                @pl.when(i < 2)
                def _():
                    wait(o_copies(slot, i + 2, *runs[0]))

            compute(i, lo, width, ((0, first), (first, width - first)), k)
            return 0

        lax.fori_loop(0, 4, tile, 0)

    def run(k, _):
        lo = (k - 1) * c
        w_slot = lax.rem(k, 2)
        at_point(k, None)
        for k0 in range(2, len(runs)):

            @pl.when(k == k0)
            def _(k0=k0):
                wait(load(k0))

        def tile(i, _):
            at_point(k, i)
            slot = lax.rem(i, 2)

            @pl.when(i >= 2)
            def _():
                wait(o_copies(slot, i - 2, lo, c))

            @pl.when(jnp.logical_and(i < 2, k == 2))
            def _():
                wait(o_copies(slot, i + 2, *runs[1]))

            @pl.when(jnp.logical_and(i < 2, k > 2))
            def _():
                wait(o_copies(slot, i + 2, lo - c, c))

            compute(i, lo, c, pieces(c), w_slot)
            return 0

        lax.fori_loop(0, 4, tile, 0)
        return 0

    lax.fori_loop(2, len(runs), run, 0)
    last = len(runs) - 1
    wait(load_d())
    before = {
        0: lambda: h3(g1),
        3: lambda: h2(u1),
        4: lambda: h3(u1),
        5: lambda: h1(d1),
    }

    def norm_of(m):
        wide = ho_v[lax.rem(m, 2)].astype(F32)
        ao_v[lax.rem(m, 2)] = (wide * scale_of(wide)).astype(BF)

    def tile(m, _):
        slot = lax.rem(m, 2)

        @pl.when(m == 3)
        def _():
            wait(o_copies(0, 2, *runs[last]))
            wait(o_copies(1, 3, *runs[last]))

        @pl.when(m < 7)
        def _():
            start(i_copies(m + 1))

        for m0, do in before.items():
            guarded(m == m0, do)
        wait(i_copies(m))

        @pl.when(m > 1)
        def _():
            wait(h_copy(m - 2))

        @pl.when(m > 2)
        def _():
            wait(a1_copy(m - 3))

        norm_of(m + 1)
        ho_v[slot] = (xi_v[slot].astype(F32) + dot(hi_v[slot], wd_v[...]).astype(BF).astype(F32)).astype(BF)
        start(h_copy(m))

        @pl.when(m > 0)
        def _():
            start(a1_copy(m - 1))

        return 0

    lax.fori_loop(0, 8, tile, 0)
    wait(a1_copy(5))
    norm_of(7)
    start(a1_copy(7))
    wait(h_copy(6))
    wait(h_copy(7))
    wait(a1_copy(6))
    wait(a1_copy(7))
    for i in range(8):
        wait(a_copy(i))
    h2(d1)
    h3(d1)


def forward(x, wg, wu, wd):
    t, d = x.shape
    f = wg.shape[2]
    c = f // CHUNKS
    n, dma = 2 * CHUNKS + 6, pltpu.SemaphoreType.DMA
    shapes = [((t, d), BF), ((t, f), BF), ((t, f), F32), ((t, f), F32), ((t, d), BF), ((t, d), BF)]
    shapes += [((2, d, f), BF), ((2, d, f), BF), ((2, f, d), BF)]
    return pl.pallas_call(
        forward_kernel,
        in_specs=[ANY] * 4,
        out_specs=[ANY] * len(shapes),
        out_shape=[jax.ShapeDtypeStruct(*s) for s in shapes],
        scratch_shapes=[
            pltpu.VMEM((t, d), BF),
            pltpu.VMEM((2, d, 2 * c), BF),
            pltpu.VMEM((4, t // 8, d), BF),
            pltpu.VMEM((2, t // 4, c), BF),
            pltpu.VMEM((2, t // 4, c), F32),
            pltpu.VMEM((2, t // 4, c), F32),
            pltpu.VMEM((f, d), BF),
            pltpu.VMEM((2, t // 8, f), BF),
            pltpu.VMEM((2, t // 8, d), BF),
            pltpu.VMEM((2, t // 8, d), BF),
            pltpu.VMEM((2, t // 8, d), BF),
            pltpu.VMEM(wg.shape[1:], BF),
            pltpu.VMEM(wd.shape[1:], BF),
            dma((2, n, 2)),
            dma((2, n, 3)),
            dma((2, n, 2)),
            dma((2, 2)),
            dma((2, 2)),
            dma((4,)),
            dma((8,)),
            dma((2, 3)),
            dma,
            dma((2, 2)),
            dma((2, 2)),
        ],
        compiler_params=pltpu.CompilerParams(vmem_limit_bytes=VMEM_LIMIT, collective_id=2, has_side_effects=True),
        cost_estimate=pl.CostEstimate(flops=6 * t * d * f, bytes_accessed=16 * t * f, transcendentals=t * f),
        name="forward",
    )(x, wg, wu, wd)


PARTS = 5
LATE = 2
TILES = 8
LEFT = 2


def input_gradient(f, dgu, wg, wu, h, dy, bg_v, bu_v):
    d = bg_v.shape[-1]

    def by_gate():
        bg_v[...] = dot(dgu[:, pl.ds(0, f)], wg[...], NT).astype(BF)

    def by_up():
        bu_v[...] = dot(dgu[:, pl.ds(f, f)], wu[...], NT).astype(BF)

    def rest():
        by_a = (bg_v[...].astype(F32) + bu_v[...].astype(F32)).astype(BF).astype(F32)
        wide = h[...].astype(F32)
        scale = scale_of(wide)
        by_scale = jnp.sum(by_a * wide, -1, keepdims=True)
        by_wide = (by_a * scale - (by_scale * scale * scale * scale * (1.0 / d)) * wide).astype(BF)
        return (dy[...].astype(F32) + by_wide.astype(F32)).astype(BF)

    return by_gate, by_up, rest


def backward_kernel(layer, *refs):
    saved = layer == 0
    a_hbm, h_hbm, dy_hbm, wg_hbm, wu_hbm, wd_hbm = refs[:6]
    if saved:
        g_hbm, u_hbm, hid_hbm, upper_hbm = refs[6:10]
        out_hbm, og_hbm, ou_hbm, od_hbm, od1_hbm, dgu_hbm, dwd_hbm = refs[10:17]
        refs = refs[17:]
    else:
        out_hbm, og_hbm, ou_hbm, od_hbm, dgu_hbm, dwd_hbm = refs[6:12]
        refs = refs[12:]
    (stg, buf_d, acc, buf_x, s_x, s_r, buf_r, s_g, sem_d, sem_x, sem_r, sem_g, sem_gl, free_d, free_x, free_r) = refs[:16]
    own_v, bd_v, ac_v, bx_v, sx_v, br_v, sg_v, dd, dx, dr, dg, dl, free_dd, free_dx, free_dr = refs[16:]

    t, d = a_hbm.shape
    f = wd_hbm.shape[1]
    c = f // CHUNKS
    own = d // 4
    quarter = own // 4
    own_d = f // 4
    rd = own_d // PARTS
    qd = d // 4
    me_r, x, core = here()
    partner, across, peers = neighbours()

    def d_copies():
        return [
            send(stg.at[rows((2 * k + 1 - core) * own, own), :], buf_d.at[k], (sem_d.at[0, k], sem_d.at[1, k]), partner)
            for k in range(2)
        ]

    def x_copies():
        return [send(s_x, buf_x, (sem_x.at[0], sem_x.at[1]), across)]

    def r_copies():
        return [
            send(s_r.at[rows(n * quarter, quarter), :], buf_r.at[k], (sem_r.at[0, k], sem_r.at[1, k]), p)
            for k, (n, p) in enumerate(peers)
        ]

    def g_copies(p):
        at = (rows(me_r * quarter, quarter), rows(p * c, c, 128))
        far = [
            send(s_g.at[:, pl.ds(i * c, c)], o.at[at], (sem_g.at[0, lax.rem(p, 2), i, k], sem_g.at[1, lax.rem(p, 2), i, k]), to)
            for k, (_, to) in enumerate(peers)
            for i, o in enumerate((og_hbm, ou_hbm))
        ]
        near = [pltpu.make_async_copy(s_g.at[:, pl.ds(i * c, c)], o.at[at], sem_gl.at[i]) for i, o in enumerate((og_hbm, ou_hbm))]
        return far + near

    def e0(p, first):
        if not first:
            pl.semaphore_wait(free_d, 1)
        start(d_copies())

    def e1(p, first, last):
        wait(d_copies())
        acc[lax.rem(p, 2)] = stg[rows((2 * x + core) * own, own), :].astype(F32) + buf_d[x].astype(F32)
        s_x[...] = (stg[rows((2 * (1 - x) + core) * own, own), :].astype(F32) + buf_d[1 - x].astype(F32)).astype(BF)
        if not last:
            pl.semaphore_signal(free_d, inc=1, device_id=partner, device_id_type=MESH)
        if not first:
            pl.semaphore_wait(free_x, 1)
        start(x_copies())

    def e2(p, first, last):
        wait(x_copies())
        total = acc[lax.rem(p, 2)] + buf_x[...].astype(F32)
        acc[lax.rem(p, 2)] = total
        s_r[...] = total.astype(BF)
        if not last:
            pl.semaphore_signal(free_x, inc=1, device_id=across, device_id_type=MESH)
        if not first:
            for k in range(3):
                pl.semaphore_wait(free_r.at[k], 1)
        start(r_copies())

    def e3(p, last):
        wait(r_copies())
        total = acc[lax.rem(p, 2), rows(me_r * quarter, quarter), :]
        for k in range(3):
            total = total + buf_r[k].astype(F32)
        s_g[...] = total.astype(BF)
        if not last:
            for k, (_, to) in enumerate(peers):
                pl.semaphore_signal(free_r.at[2 - k], inc=1, device_id=to, device_id_type=MESH)
        start(g_copies(p))

    def e4(p):
        wait(g_copies(p))

    late = LATE if saved else 0
    pieces_d = PARTS + late if saved else PARTS - LATE

    def source(q):
        return (upper_hbm, PARTS - late + q) if q < late else (dwd_hbm, q - late)

    def dd_far(q):
        src, part = source(q)
        n = q % 2
        return [
            send(src.at[rows((2 * m + 1 - core) * own_d + part * rd, rd), :], bd_v.at[n, m], (dd.at[0, n, m], dd.at[1, n, m]), partner)
            for m in range(2)
        ]

    def dd_near(q):
        src, part = source(q)
        n = q % 2
        return [
            pltpu.make_async_copy(src.at[rows((2 * m + core) * own_d + part * rd, rd), :], own_v.at[n, m], dl.at[0, n, m])
            for m in range(2)
        ]

    def dx_copies(q):
        n = q % 2
        return [send(sx_v.at[n], bx_v.at[n], (dx.at[0, n], dx.at[1, n]), across)]

    def dr_copies(q):
        n = q % 2
        return [
            send(sx_v.at[n, :, rows(to_r * qd, qd, 128)], br_v.at[n, m], (dr.at[0, n, m], dr.at[1, n, m]), to)
            for m, (to_r, to) in enumerate(peers)
        ]

    def dg_copies(q):
        n = q % 2
        dst, part = (od1_hbm, q) if q < late else (od_hbm, q - late)
        at = (rows(part * rd, rd), rows(me_r * qd, qd, 128))
        far = [send(sg_v.at[n], dst.at[at], (dg.at[0, n, m], dg.at[1, n, m]), to) for m, (_, to) in enumerate(peers)]
        return far + [pltpu.make_async_copy(sg_v.at[n], dst.at[at], dl.at[1, n, 0])]

    def f0(q):
        if q >= 2:
            pl.semaphore_wait(free_dd, 1)
        start(dd_far(q))
        start(dd_near(q))

    def f1(q):
        n = q % 2
        wait(dd_near(q))
        wait(dd_far(q))
        ac_v[n] = own_v[n, x].astype(F32) + bd_v[n, x].astype(F32)
        sx_v[n] = (own_v[n, 1 - x].astype(F32) + bd_v[n, 1 - x].astype(F32)).astype(BF)
        if q + 2 < pieces_d:
            pl.semaphore_signal(free_dd, inc=1, device_id=partner, device_id_type=MESH)
        if q >= 2:
            pl.semaphore_wait(free_dx, 1)
        start(dx_copies(q))

    def f2(q):
        n = q % 2
        wait(dx_copies(q))
        total = ac_v[n] + bx_v[n].astype(F32)
        ac_v[n] = total
        sx_v[n] = total.astype(BF)
        if q + 2 < pieces_d:
            pl.semaphore_signal(free_dx, inc=1, device_id=across, device_id_type=MESH)
        if q >= 2:
            for m in range(3):
                pl.semaphore_wait(free_dr.at[m], 1)
        start(dr_copies(q))

    def f3(q):
        n = q % 2
        wait(dr_copies(q))
        total = ac_v[n, :, rows(me_r * qd, qd, 128)]
        for m in range(3):
            total = total + br_v[n, m].astype(F32)
        sg_v[n] = total.astype(BF)
        if q + 2 < pieces_d:
            for m, (_, to) in enumerate(peers):
                pl.semaphore_signal(free_dr.at[2 - m], inc=1, device_id=to, device_id_type=MESH)
        start(dg_copies(q))

    def f4(q):
        wait(dg_copies(q))

    def do(*events):
        for event in events:
            event()

    E0 = lambda p: lambda: e0(p, p == 0)
    E1 = lambda p: lambda: e1(p, p == 0, p == CHUNKS - 1)
    E2 = lambda p: lambda: e2(p, p == 0, p == CHUNKS - 1)
    E3 = lambda p: lambda: e3(p, p == CHUNKS - 1)
    E4 = lambda p: lambda: e4(p)
    F0, F1, F2, F3, F4 = (lambda q, g=g: lambda: g(q) for g in (f0, f1, f2, f3, f4))

    tm = t // 4
    tiles = t // tm
    if saved:
        at_start = {0: [F0(0), F0(1)], 1: [F1(0), F1(1)], 3: [F2(0)], 4: [F2(1)]}
        at_chunk = {
            (0, 0): [F3(0)],
            (0, 1): [F3(1), F0(2), F0(3)],
            (0, 3): [F1(2), F1(3)],
            (0, 4): [F4(0), F4(1)],
            (1, 0): [F2(2), E0(0), F0(4)],
            (1, 2): [F2(3), E1(0)],
            (1, 4): [F3(2), F1(4)],
            (2, 0): [F3(3), F4(2), E0(1), F0(5)],
            (2, 1): [E2(0)],
            (2, 2): [E1(1)],
            (2, 4): [F2(4), F1(5)],
            (3, 0): [F3(4), F4(3), E3(0), E0(2), F0(6)],
            (3, 1): [E2(1)],
            (3, 2): [E1(2)],
            (3, 4): [F4(4), F2(5), F1(6)],
            (4, 0): [E4(0), E3(1), E0(3)],
            (4, 2): [F3(5), E2(2), E1(3)],
        }
        at_end = {
            -1: [E0(4), E4(1), E3(2), F2(6)],
            0: [E2(3), E1(4)],
            1.5: [F4(5), F3(6), E4(2)],
            2.5: [E3(3), E2(4)],
            4: [F4(6), E4(3)],
            5: [E3(4)],
        }
        after = [E4(4)]
    else:
        at_start = {}
        at_chunk = {
            (1, 0): [E0(0)],
            (1, 2): [E1(0)],
            (2, 0): [E2(0), E0(1)],
            (2, 2): [E1(1)],
            (2, 4): [E3(0)],
            (3, 0): [E4(0), E2(1), E0(2)],
            (3, 2): [E1(2)],
            (3, 4): [E3(1)],
            (4, 0): [E4(1), E2(2), E0(3)],
            (4, 2): [E1(3)],
            (4, 4): [E3(2)],
        }
        at_end = {
            -1: [E4(2), E2(3), E0(4), F0(0), F0(1)],
            0: [E1(4)],
            0.5: [F1(0), F1(1), F0(2)],
            1: [E3(3)],
            2: [E2(4)],
            3: [F2(0), E4(3)],
            3.5: [E3(4)],
            4: [F3(0), F2(1), F1(2)],
            5.5: [F4(0), F2(2)],
            6: [F3(1), E4(4)],
            6.5: [F3(2)],
        }
        after = [F4(1), F4(2)]

    def chunks(*bufs):
        if saved:
            a_v, dy_v, wd_v, dgs, dst, g_v, u_v, sem_a, sem_w, sem_o, sem_s, sem_h = bufs
        else:
            a_v, dy_v, wd_v, hid_v, dgs, dst, wgu_v, sem_a, sem_w, sem_o = bufs

        def a_copy(i):
            at = rows(i * tm, tm)
            return [pltpu.make_async_copy(a_hbm.at[at, :], a_v.at[at, :], sem_a.at[0, i])]

        def dy_copy(i):
            at = rows(i * tm, tm)
            return [pltpu.make_async_copy(dy_hbm.at[at, :], dy_v.at[at, :], sem_a.at[1, i])]

        def w_copies(j):
            at = rows(j * c, c, 128)
            w = [pltpu.make_async_copy(wd_hbm.at[layer, at, :], wd_v, sem_w.at[0])]
            if not saved:
                w.append(pltpu.make_async_copy(wg_hbm.at[layer, :, at], wgu_v.at[:, pl.ds(0, c)], sem_w.at[1]))
                w.append(pltpu.make_async_copy(wu_hbm.at[layer, :, at], wgu_v.at[:, pl.ds(c, c)], sem_w.at[2]))
            return w

        def s_copies(n):
            slot = lax.rem(n, 2)
            at = (rows(lax.rem(n, tiles) * tm, tm), rows(lax.div(n, tiles) * c, c, 128))
            return [
                pltpu.make_async_copy(g_hbm.at[at], g_v.at[slot], sem_s.at[slot, 0]),
                pltpu.make_async_copy(u_hbm.at[at], u_v.at[slot], sem_s.at[slot, 1]),
            ]

        def o_copies(j):
            return [
                pltpu.make_async_copy(dgs.at[:, pl.ds(0, c)], dgu_hbm.at[:, rows(j * c, c, 128)], sem_o.at[0]),
                pltpu.make_async_copy(dgs.at[:, pl.ds(c, c)], dgu_hbm.at[:, rows(f + j * c, c, 128)], sem_o.at[1]),
            ]

        def hid_copy(k):
            half = lax.rem(k, 2)
            return [pltpu.make_async_copy(hid_hbm.at[:, rows(k * c, c, 128)], dgs.at[:, rows(half * c, c, 128)], sem_h.at[half])]

        def dw_copy(j):
            n = lax.rem(j, 2) if saved else 0
            return [pltpu.make_async_copy(dst.at[n], dwd_hbm.at[rows(j * c, c), :], sem_o.at[2 + n])]

        everyone = [partner, across] + [p for _, p in peers]
        if saved:
            start(hid_copy(0))
            for i in range(tiles):
                start(dy_copy(i))
            meet(everyone)
            start(hid_copy(1))
            start(w_copies(0))
            start(s_copies(0))
            for i in range(tiles):
                start(a_copy(i))
            for i in range(tiles):
                wait(dy_copy(i))

            def down(k, _):
                half = lax.rem(k, 2)
                wait(hid_copy(k))
                for k0, events in at_start.items():
                    guarded(k == k0, lambda events=events: do(*events))

                @pl.when(k >= 2)
                def _():
                    wait(dw_copy(k - 2))

                for p0, w in pieces(c):
                    dst[half, pl.ds(p0, w), :] = dot(dgs[:, rows(half * c + p0, w, 128)], dy_v[...], TN).astype(BF)
                start(dw_copy(k))

                @pl.when(k + 2 < CHUNKS)
                def _():
                    start(hid_copy(k + 2))

                return 0

            lax.fori_loop(0, CHUNKS, down, 0)
            wait(dw_copy(CHUNKS - 2))
            wait(dw_copy(CHUNKS - 1))
            for i in range(tiles):
                wait(a_copy(i))
        else:
            start(w_copies(0))
            for i in range(tiles):
                start(a_copy(i))
                start(dy_copy(i))
            meet(everyone)

        def events_at(j, point):
            for (j0, point0), events in at_chunk.items():
                if isinstance(point, int):
                    if point == point0:
                        guarded(j == j0, lambda events=events: do(*events))
                elif point0 < 4:
                    guarded(jnp.logical_and(j == j0, point == point0), lambda events=events: do(*events))

        def chunk(j, _):
            @pl.when(j >= 1)
            def _():
                wait(o_copies(j - 1))

            wait(w_copies(j))

            def tile(i, _):
                if saved:
                    n = j * tiles + i

                    @pl.when(n + 1 < CHUNKS * tiles)
                    def _():
                        start(s_copies(n + 1))

                    wait(s_copies(n))
                else:

                    @pl.when(j == 0)
                    def _():
                        wait(a_copy(i))
                        wait(dy_copy(i))

                events_at(j, i)
                r = rows(i * tm, tm)
                for p0, w in pieces(c):
                    if not saved:
                        a = a_v[r, :]
                        both = dot(a, jnp.concatenate([wgu_v[:, pl.ds(p0, w)], wgu_v[:, pl.ds(c + p0, w)]], 1))
                        g, u = both[:, :w], both[:, w:]
                    dh = dot(dy_v[r, :], wd_v[pl.ds(p0, w), :], NT).astype(BF).astype(F32)
                    if saved:
                        by_gate, by_up = g_v[lax.rem(n, 2), :, pl.ds(p0, w)], u_v[lax.rem(n, 2), :, pl.ds(p0, w)]
                    else:
                        s = jax.nn.sigmoid(g)
                        by_up = g * s
                        by_gate = u * (s + by_up * (1.0 - s))
                        hid_v[r, pl.ds(p0, w)] = (by_up * u).astype(BF)
                    dgs[r, pl.ds(c + p0, w)] = (dh * by_up).astype(BF)
                    dgs[r, pl.ds(p0, w)] = (dh * by_gate).astype(BF)
                return 0

            lax.fori_loop(0, tiles, tile, 0)
            start(o_copies(j))

            @pl.when(j + 1 < CHUNKS)
            def _():
                start(w_copies(j + 1))

            events_at(j, 4)
            if not saved:

                @pl.when(j >= 1)
                def _():
                    wait(dw_copy(j - 1))

                for p0, w in pieces(c):
                    dst[0, pl.ds(p0, w), :] = dot(hid_v[:, pl.ds(p0, w)], dy_v[...], TN).astype(BF)
                start(dw_copy(j))
            for k in range(2):
                stg[pl.ds(k * (d // 2), d // 2), :] = dot(a_v[:, pl.ds(k * (d // 2), d // 2)], dgs[...], TN).astype(BF)
            return 0

        lax.fori_loop(0, CHUNKS, chunk, 0)
        wait(o_copies(CHUNKS - 1))
        if not saved:
            wait(dw_copy(CHUNKS - 1))

    dma = pltpu.SemaphoreType.DMA
    bufs = [pltpu.VMEM((t, d), BF), pltpu.VMEM((t, d), BF), pltpu.VMEM((c, d), BF)]
    bufs += [] if saved else [pltpu.VMEM((t, c), BF)]
    bufs += [pltpu.VMEM((t, 2 * c), BF), pltpu.VMEM((2 if saved else 1, c, d), BF)]
    bufs += [pltpu.VMEM((2, tm, c), F32)] * 2 if saved else [pltpu.VMEM((d, 2 * c), BF)]
    bufs += [dma((2, tiles)), dma((3,)), dma((4,))]
    bufs += [dma((2, 2)), dma((2,))] if saved else []
    pl.run_scoped(chunks, *bufs)

    ta = t // TILES
    count = TILES - LEFT if saved else TILES

    def last(wg_v, wu_v, dgu_v, h_v, dy_v, o_v, bg_v, bu_v, sem_w, sem_i, sem_o):
        def i_copy(i, m):
            slot = lax.rem(i, 2)
            part = pl.ds(m * f, f)
            return [pltpu.make_async_copy(dgu_hbm.at[rows(i * ta, ta), part], dgu_v.at[slot, :, part], sem_i.at[slot, m])]

        def h_copies(i):
            slot = lax.rem(i, 2)
            at = rows(i * ta, ta)
            return [
                pltpu.make_async_copy(h_hbm.at[at, :], h_v.at[slot], sem_i.at[slot, 2]),
                pltpu.make_async_copy(dy_hbm.at[at, :], dy_v.at[slot], sem_i.at[slot, 3]),
            ]

        def o_copy(i):
            slot = lax.rem(i, 2)
            return [pltpu.make_async_copy(o_v.at[slot], out_hbm.at[rows(i * ta, ta), :], sem_o.at[slot])]

        def w_copy(k):
            return [pltpu.make_async_copy((wg_hbm, wu_hbm)[k].at[layer], (wg_v, wu_v)[k], sem_w.at[k])]

        def work(i):
            n = lax.rem(i, 2)
            return input_gradient(f, dgu_v.at[n], wg_v, wu_v, h_v.at[1 - n], dy_v.at[1 - n], bg_v, bu_v)

        start(w_copy(0))
        start(i_copy(0, 0))
        start(w_copy(1))
        start(i_copy(0, 1))
        start(h_copies(0))
        do(*at_end[-1])

        def events_at(i, half):
            for point, events in at_end.items():
                if point >= 0 and point % 1 == half:
                    guarded(i == int(point), lambda events=events: do(*events))

        def tile(i, _):
            @pl.when(i + 1 < count)
            def _():
                start(i_copy(i + 1, 0))
                start(i_copy(i + 1, 1))

            @pl.when(i == 0)
            def _():
                wait(w_copy(0))

            wait(i_copy(i, 0))

            @pl.when(i >= 1)
            def _():
                start(h_copies(i))
                wait(h_copies(i - 1))

            @pl.when(i >= 3)
            def _():
                wait(o_copy(i - 3))

            events_at(i, 0)
            by_gate, by_up, rest = work(i)
            o_v[lax.rem(i + 1, 2)] = rest()
            by_gate()

            @pl.when(i >= 1)
            def _():
                start(o_copy(i - 1))

            @pl.when(i == 0)
            def _():
                wait(w_copy(1))

            wait(i_copy(i, 1))
            events_at(i, 0.5)
            by_up()
            return 0

        lax.fori_loop(0, count, tile, 0)
        wait(h_copies(count - 1))
        wait(o_copy(count - 3))
        _, _, rest = work(count)
        o_v[(count - 1) % 2] = rest()
        start(o_copy(count - 1))
        wait(o_copy(count - 2))
        wait(o_copy(count - 1))
        do(*after)

    pl.run_scoped(
        last,
        pltpu.VMEM((d, f), BF),
        pltpu.VMEM((d, f), BF),
        pltpu.VMEM((2, ta, 2 * f), BF),
        pltpu.VMEM((2, ta, d), BF),
        pltpu.VMEM((2, ta, d), BF),
        pltpu.VMEM((2, ta, d), BF),
        pltpu.VMEM((ta, d), BF),
        pltpu.VMEM((ta, d), BF),
        dma((2,)),
        dma((2, 4)),
        dma((2,)),
    )


def backward(a, h, dy, wg, wu, wd, saved, layer):
    t, d = a.shape
    f = wd.shape[1]
    c = f // CHUNKS
    own, rd, dma = d // 4, f // 4 // PARTS, pltpu.SemaphoreType.DMA
    regular = pltpu.SemaphoreType.REGULAR
    shapes = [(t, d), (own, f), (own, f), (f // 4, d)] + ([(LATE * rd, d)] if saved else []) + [(t, 2 * f), (f, d)]
    return pl.pallas_call(
        functools.partial(backward_kernel, layer),
        in_specs=[ANY] * (6 + len(saved)),
        out_specs=[ANY] * len(shapes),
        out_shape=[jax.ShapeDtypeStruct(s, BF) for s in shapes],
        scratch_shapes=[
            pltpu.VMEM((d, 2 * c), BF),
            pltpu.VMEM((2, own, 2 * c), BF),
            pltpu.VMEM((2, own, 2 * c), F32),
            pltpu.VMEM((own, 2 * c), BF),
            pltpu.VMEM((own, 2 * c), BF),
            pltpu.VMEM((own, 2 * c), BF),
            pltpu.VMEM((3, own // 4, 2 * c), BF),
            pltpu.VMEM((own // 4, 2 * c), BF),
            dma((2, 2)),
            dma((2,)),
            dma((2, 3)),
            dma((2, 2, 2, 3)),
            dma((2,)),
            regular,
            regular,
            regular((3,)),
            pltpu.VMEM((2, 2, rd, d), BF),
            pltpu.VMEM((2, 2, rd, d), BF),
            pltpu.VMEM((2, rd, d), F32),
            pltpu.VMEM((2, rd, d), BF),
            pltpu.VMEM((2, rd, d), BF),
            pltpu.VMEM((2, 3, rd, d // 4), BF),
            pltpu.VMEM((2, rd, d // 4), BF),
            dma((2, 2, 2)),
            dma((2, 2)),
            dma((2, 2, 3)),
            dma((2, 2, 3)),
            dma((2, 2, 2)),
            regular,
            regular,
            regular((3,)),
        ],
        compiler_params=pltpu.CompilerParams(vmem_limit_bytes=VMEM_LIMIT, collective_id=layer, has_side_effects=True),
        cost_estimate=pl.CostEstimate(flops=(12 if saved else 16) * t * d * f, bytes_accessed=30 * t * f, transcendentals=t * f),
        name=f"backward_{layer}",
    )(a, h, dy, wg, wu, wd, *saved)


def last_kernel(n_sums, f, *refs):
    by_x, dgu, wg, wu, h, dy = refs[:6]
    sums = refs[6 : 6 + n_sums]
    outs = refs[6 + n_sums : 10 + n_sums]
    wg_v, wu_v, dgu_v, h_v, dy_v, o_v, bg_v, bu_v, x_v, *rest = refs[10 + n_sums :]
    bufs, (sem_w, sem_i, sem_o, sem_in, sem_out) = rest[:n_sums], rest[n_sums:]
    t, d = by_x.shape
    ta = t // TILES
    count = TILES - LEFT

    def i_copy(i, m):
        at, part = rows((count + i) * ta, ta), pl.ds(m * f, f)
        return pltpu.make_async_copy(dgu.at[at, part], dgu_v.at[i, :, part], sem_i.at[i, m])

    def h_copies(i):
        at = rows((count + i) * ta, ta)
        return [
            pltpu.make_async_copy(h.at[at, :], h_v.at[i], sem_i.at[i, 2]),
            pltpu.make_async_copy(dy.at[at, :], dy_v.at[i], sem_i.at[i, 3]),
        ]

    def o_copy(i):
        return pltpu.make_async_copy(o_v.at[i], outs[0].at[rows((count + i) * ta, ta), :], sem_o.at[i])

    w_copies = [pltpu.make_async_copy(w.at[0], v, sem_w.at[k]) for k, (w, v) in enumerate(((wg, wg_v), (wu, wu_v)))]
    w_copies[0].start()
    i_copy(0, 0).start()
    w_copies[1].start()
    i_copy(0, 1).start()
    moves = [(by_x.at[pl.ds(i * ta, ta), :], x_v.at[pl.ds(i * ta, ta), :], outs[0].at[pl.ds(i * ta, ta), :]) for i in range(count)]
    at = [(1, 0, 0), (1, 1, 0), (2, 0, 0), (2, 1, 0), (3, 0, 0), (3, 1, 0), (3, 1, outs[3].shape[1] - sums[6].shape[0])]
    for src, buf, (o, layer, lo) in zip(sums, bufs, at, strict=True):
        size = outs[o].shape[1] - sums[6].shape[0] if (o, layer, lo) == (3, 1, 0) else src.shape[0]
        moves.append((src.at[pl.ds(0, size), :], buf.at[pl.ds(0, size), :], outs[o].at[layer, pl.ds(lo, size), :]))
    moves = [
        (pltpu.make_async_copy(src, buf, sem_in.at[k]), pltpu.make_async_copy(buf, dst, sem_out.at[k]))
        for k, (src, buf, dst) in enumerate(moves)
    ]
    def take(n):
        for first, _ in moves[n :: 2 * LEFT]:
            first.start()

    def give(n):
        for first, second in moves[n :: 2 * LEFT]:
            first.wait()
            second.start()

    def tile(i, _):
        by_gate, by_up, rest = input_gradient(f, dgu_v.at[i], wg_v, wu_v, h_v.at[i], dy_v.at[i], bg_v, bu_v)

        @pl.when(i == 0)
        def _():
            w_copies[0].wait()

        i_copy(i, 0).wait()
        for n in range(LEFT):

            @pl.when(i == n)
            def _(n=n):
                if n > 0:
                    give(2 * n - 1)
                take(2 * n)

        by_gate()

        @pl.when(i == 0)
        def _():
            w_copies[1].wait()

        i_copy(i, 1).wait()
        for n in range(LEFT):

            @pl.when(i == n)
            def _(n=n):
                give(2 * n)
                start(h_copies(n))
                take(2 * n + 1)
                if n + 1 < LEFT:
                    i_copy(n + 1, 0).start()
                    i_copy(n + 1, 1).start()

        by_up()
        wait(h_copies(i))
        o_v[i] = rest()
        o_copy(i).start()
        return 0

    lax.fori_loop(0, LEFT, tile, 0)
    give(2 * LEFT - 1)
    for i in range(LEFT):
        o_copy(i).wait()
    for _, second in moves:
        second.wait()


def finish(by_x, dgu, wg, wu, h, dy, *sums):
    t, d = by_x.shape
    f = wg.shape[2]
    ta = t // TILES
    outs = [(t, d)] + [(2, *sums[n].shape) for n in (0, 2, 4)]
    tile, dma = pltpu.VMEM((LEFT, ta, d), BF), pltpu.SemaphoreType.DMA
    moves = TILES - LEFT + len(sums)
    return pl.pallas_call(
        functools.partial(last_kernel, len(sums), f),
        in_specs=[ANY] * (6 + len(sums)),
        out_specs=[ANY] * len(outs),
        out_shape=[jax.ShapeDtypeStruct(s, BF) for s in outs],
        scratch_shapes=[pltpu.VMEM((d, f), BF), pltpu.VMEM((d, f), BF), pltpu.VMEM((LEFT, ta, 2 * f), BF)]
        + [tile] * 3
        + [pltpu.VMEM((ta, d), BF)] * 2
        + [pltpu.VMEM(((TILES - LEFT) * ta, d), BF)]
        + [pltpu.VMEM(s.shape, BF) for s in sums]
        + [dma((2,)), dma((LEFT, 4)), dma((LEFT,)), dma((moves,)), dma((moves,))],
        compiler_params=pltpu.CompilerParams(vmem_limit_bytes=VMEM_LIMIT),
        cost_estimate=pl.CostEstimate(flops=4 * LEFT * ta * d * f, bytes_accessed=16 * t * d, transcendentals=0),
        name="finish",
    )(by_x, dgu, wg, wu, h, dy, *sums)


def solution(mesh):
    def step(x, dy, *weights):
        x, dy = x[0], dy[0]
        a0, hid, g, u, h, a1, *whole = forward(x, *weights)
        by_h, g1, u1, d1, _, upper = backward(a1, h, dy, *whole, (), 1)
        by_x, g0, u0, d0, d1_late, dgu, _ = backward(a0, x, by_h, *whole, (g, u, hid, upper), 0)
        by_x, *sums = finish(by_x, dgu, *whole[:2], x, by_h, g0, g1, u0, u1, d0, d1, d1_late)
        return (by_x[None], *sums)

    states, cut = P(("rep", "r", "s"), None, None), P(None, "s", None)
    return jax.shard_map(
        step,
        mesh=mesh,
        in_specs=(states, states) + (cut,) * 3,
        out_specs=(states,) + (P("rep", "s", None),) * 3,
        check_vma=False,
    )
```
